32 devices in a mesh: gx: 2 (over y), gy: 4 (over z), gz: 4 (over x, core).
Axes of the slice: x: 2, y: 2, z: 4, core: 2. Of those that a mesh axis runs over, the one named last changes fastest.
Arguments:
- density: float32 [24, 64, 512], P('gx', 'gy', 'gz'), may hold values from 0.5 to 8
- potential: float32 [24, 64, 512], P('gx', 'gy', 'gz'), may hold values from -6 to 6
Outputs:
- corrected: float32 [24, 64, 512], P('gx', 'gy', 'gz')
The draws below stay inside these ranges and needn't reach their ends.
All inputs are finite; a program needn't handle non-finite values.
Results may differ from the reference program's by a relative error of at most 0.00005.
Values sent between devices are 32-bit elements; how exact they have to be, the bound alone decides.
A program may use at most 64 MiB of HBM per device.

```python
import math
import jax
import jax.numpy as jnp
from jax import lax

CX = 12
CY = 16
CZ = 128
SWEEPS = 2
NX = 24
NY = 64
NZ = 512
N_GX = 2
N_GY = 4
N_GZ = 4


def levels(stream_key, shape, split, low, top_value):
    factor_of = 1.0
    for dim, shards_of in split:
        steps = jax.random.uniform(jax.random.fold_in(jax.random.fold_in(stream_key, 6), dim), (shards_of,), jnp.float32, low / len(split), top_value / len(split))
        factor_of = factor_of * jnp.repeat(jnp.exp(steps), shape[dim] // shards_of).reshape((-1,) + (1,) * (len(shape) - 1 - dim))
    return factor_of


def normal_values(rng, shape, width, bound, split=(), kind=jnp.bfloat16):
    level = levels(rng, shape, split, -0.22, 0.18) if split else 1.0
    entries = jax.random.normal(rng, shape, jnp.float32) * width * level
    return jnp.minimum(jnp.maximum(entries, -bound), bound).astype(kind)


def setup_inputs(seed: int = 0) -> dict:
    splits = jax.random.split(jax.random.key(seed), 3)
    return {
        "density": jnp.clip(jnp.exp(math.log(8.0) - 2.7725887 * jax.random.uniform(splits[0], (NX, NY, NZ), jnp.float32) ** levels(splits[0], (NX, NY, NZ), ((0, 2), (1, 4), (2, 4)), -0.2, 0.2)), 0.5, 8.0),
        "potential": normal_values(splits[1], (NX, NY, NZ), 1.0, 6.0, ((0, 2), (1, 4), (2, 4)), jnp.float32),
    }


def beside_all(field):
    total = jnp.roll(field, -1, 0) + jnp.roll(field, 1, 0)
    total = total + jnp.roll(field, -1, 1) + jnp.roll(field, 1, 1)
    return total + jnp.roll(field, -1, 2) + jnp.roll(field, 1, 2)

def colour(shape, offset):
    summed = lax.broadcasted_iota(jnp.int32, shape, 0) + lax.broadcasted_iota(jnp.int32, shape, 1)
    summed = summed + lax.broadcasted_iota(jnp.int32, shape, 2) + offset
    return summed % 2 == 0

def smooth(field, source, red):
    field = jnp.where(red, (beside_all(field) - source) / 6.0, field)
    return jnp.where(red, field, (beside_all(field) - source) / 6.0)

def basis(count):
    rows = lax.broadcasted_iota(jnp.int32, (count, count), 0).astype(jnp.float32)
    cols = lax.broadcasted_iota(jnp.int32, (count, count), 1)
    freq = ((cols + 1) // 2).astype(jnp.float32)
    angle = 2.0 * jnp.pi * freq * rows / count
    full = jnp.sqrt(2.0 / count)
    single = 1.0 / jnp.sqrt(jnp.float32(count))
    top = 2 * ((cols + 1) // 2) == count
    table = jnp.where(cols % 2 == 1, jnp.cos(angle) * full, jnp.sin(angle) * full)
    table = jnp.where(top, jnp.cos(angle) * single, table)
    table = jnp.where(cols == 0, single, table)
    modes = ((jnp.arange(count, dtype=jnp.int32) + 1) // 2).astype(jnp.float32)
    return (table, 2.0 - 2.0 * jnp.cos(2.0 * jnp.pi * modes / count))

def coarse_solve(blocks, weight_x, weight_y, weight_z):
    nx, ny, nz = blocks.shape
    qx, lx = basis(nx)
    qy, ly = basis(ny)
    qz, lz = basis(nz)
    hi = lax.Precision.HIGHEST
    spectrum = jnp.einsum('ia,jb,kc,ijk->abc', qx, qy, qz, blocks, precision=hi)
    denom = weight_x * lx[:, None, None] + weight_y * ly[None, :, None] + weight_z * lz[None, None, :]
    zero = colour((nx, ny, nz), 0) & (lax.broadcasted_iota(jnp.int32, (nx, ny, nz), 0) + lax.broadcasted_iota(jnp.int32, (nx, ny, nz), 1) + lax.broadcasted_iota(jnp.int32, (nx, ny, nz), 2) == 0)
    safe = jnp.where(zero, jnp.float32(1.0), denom)
    spectrum = jnp.where(zero, jnp.float32(0.0), -spectrum / safe)
    return jnp.einsum('ia,jb,kc,abc->ijk', qx, qy, qz, spectrum, precision=hi)

def widen(field, bx, by, bz):
    return jnp.repeat(jnp.repeat(jnp.repeat(field, bx, 0), by, 1), bz, 2)

def reference(density, potential):
    source = density - jnp.sum(density) / (NX * NY * NZ)
    red = colour(source.shape, 0)
    fine = potential
    for sweep in range(SWEEPS):
        fine = smooth(fine, source, red)
    left = source - (beside_all(fine) - 6.0 * fine)
    level_one = left.reshape(NX // 2, 2, NY // 2, 2, NZ // 2, 2).sum(axis=(1, 3, 5)) * 0.5
    red_one = colour(level_one.shape, 0)
    error_one = jnp.zeros_like(level_one)
    for sweep in range(SWEEPS):
        error_one = smooth(error_one, level_one, red_one)
    rest = level_one - (beside_all(error_one) - 6.0 * error_one)
    bx, by, bz = (CX // 2, CY // 2, CZ // 2)
    blocks = rest.reshape(N_GX, bx, N_GY, by, N_GZ, bz).sum(axis=(1, 3, 5))
    coarse = coarse_solve(blocks, float(by * bz), float(bx * bz), float(bx * by))
    error_one = error_one + widen(coarse, bx, by, bz)
    for sweep in range(SWEEPS):
        error_one = smooth(error_one, level_one, red_one)
    fine = fine + widen(error_one, 2, 2, 2)
    for sweep in range(SWEEPS):
        fine = smooth(fine, source, red)
    return fine
```

```python
import functools
import numpy as np
import jax
import jax.numpy as jnp
from jax import lax
from jax.experimental import pallas as pl
from jax.experimental.pallas import tpu as pltpu
from jax.sharding import PartitionSpec as P

SWEEPS = 2
HI = lax.Precision.HIGHEST
MESH = pl.DeviceIdType.MESH
R = 8


def table(count):
    modes = (np.arange(count) + 1) // 2
    angle = 2 * np.pi * np.outer(np.arange(count), modes) / count
    q = np.where(np.arange(count) % 2 == 1, np.cos(angle), np.sin(angle)) * np.sqrt(2 / count)
    q = np.where(2 * modes == count, np.cos(angle) / np.sqrt(count), q)
    q[:, 0] = 1 / np.sqrt(count)
    return q, 2 - 2 * np.cos(2 * np.pi * modes / count)


def coarse_operator(nx, ny, nz, wx, wy, wz):
    qx, lx = table(nx)
    qy, ly = table(ny)
    qz, lz = table(nz)
    q = np.kron(np.kron(qx, qy), qz)
    lam = wx * lx[:, None, None] + wy * ly[None, :, None] + wz * lz[None, None, :]
    lam = lam.reshape(-1)
    inv = np.concatenate([[0.0], -1.0 / lam[1:]])
    return ((q * inv) @ q.T).astype(np.float32)


def kernel(
    dims, den_hbm, pot_hbm, op_ref, sz_ref, sy_ref, rz_ref, ry_ref, out_ref,
    pa, pb, den, lv, ea, eb, e2, f2, gat, cv,
    pk_p, pk_d, pk_l, pk_e, pk_f, rk_p, rk_d, rk_l, rk_e, rk_f,
    ssem, rsem, gs, gr, lsem,
):
    nx, ny, nz, X, Y, Z = dims
    n = nx * ny * nz
    x1, y1, z1 = X // 2, Y // 2, Z // 2
    ix, iy, iz = lax.axis_index("gx"), lax.axis_index("gy"), lax.axis_index("gz")
    me = (ix * ny + iy) * nz + iz

    def device(o):
        ox, oy, oz = o // (ny * nz), (o // nz) % ny, o % nz
        return (lax.rem(ix + ox, nx), lax.rem(iy + oy, ny), lax.rem(iz + oz, nz))

    load_p = pltpu.make_async_copy(pot_hbm, pa.at[pl.ds(5, X), pl.ds(R, Y), pl.ds(0, Z)], lsem.at[0])
    load_d = pltpu.make_async_copy(den_hbm, den.at[pl.ds(5, X), pl.ds(R, Y), pl.ds(0, Z)], lsem.at[1])
    load_p.start()
    load_d.start()

    barrier = pltpu.get_barrier_semaphore()

    def greet(o, carry):
        pl.semaphore_signal(barrier, inc=1, device_id=device(o), device_id_type=MESH)
        return carry

    lax.fori_loop(1, n, greet, 0)
    pl.semaphore_wait(barrier, n - 1)
    load_p.wait()
    load_d.wait()

    sems = iter(range(60))

    def send(src, dst, step):
        k = next(sems)
        to = {
            0: (lax.rem(ix + step + nx, nx), iy, iz),
            1: (ix, lax.rem(iy + step + ny, ny), iz),
            2: (ix, iy, lax.rem(iz + step + nz, nz)),
        }[send.axis]
        copy = pltpu.make_async_remote_copy(
            src_ref=src, dst_ref=dst, send_sem=ssem.at[k], recv_sem=rsem.at[k],
            device_id=to, device_id_type=MESH,
        )
        copy.start()
        return copy

    def exchange(items):
        send.axis = 0
        copies = []
        for buf, h, H, (sx, sy, sz), pk, rk in items:
            rows, lanes = pl.ds(R, sy), pl.ds(0, 128)
            copies.append(send(buf.at[pl.ds(H + sx - h, h), rows, lanes], buf.at[pl.ds(H - h, h), rows, lanes], 1))
            copies.append(send(buf.at[pl.ds(H, h), rows, lanes], buf.at[pl.ds(H + sx, h), rows, lanes], -1))
        for copy in copies:
            copy.wait()
        send.axis = 1
        copies = []
        for buf, h, H, (sx, sy, sz), pk, rk in items:
            planes, lanes = pl.ds(H - h, sx + 2 * h), pl.ds(0, 128)
            copies.append(send(buf.at[planes, pl.ds(sy, R), lanes], buf.at[planes, pl.ds(0, R), lanes], 1))
            copies.append(send(buf.at[planes, pl.ds(R, R), lanes], buf.at[planes, pl.ds(R + sy, R), lanes], -1))
        for copy in copies:
            copy.wait()
        send.axis = 2
        copies = []
        for buf, h, H, (sx, sy, sz), pk, rk in items:
            rows = sy + 2 * R
            lane = lax.broadcasted_iota(jnp.int32, (rows, 128), 1)
            head = tail = jnp.zeros((rows, 128), jnp.float32)
            for q in range(sx + 2 * h):
                v = buf[H - h + q, :, 0:128]
                inside = (lane >= q * h) & (lane < q * h + h)
                tail = jnp.where(inside, pltpu.roll(v, (q * h - (sz - h)) % 128, 1), tail)
                head = jnp.where(inside, pltpu.roll(v, q * h, 1) if q else v, head)
            pk[0] = tail
            pk[1] = head
            copies.append(send(pk.at[0], rk.at[0], 1))
            copies.append(send(pk.at[1], rk.at[1], -1))
        for copy in copies:
            copy.wait()
        for buf, h, H, (sx, sy, sz), pk, rk in items:
            rows = sy + 2 * R
            lane = lax.broadcasted_iota(jnp.int32, (rows, 128), 1)
            left, right = rk[0], rk[1]
            wide = sz == 128
            at = 0 if wide else sz
            for q in range(sx + 2 * h):
                a = pltpu.roll(left, (128 - h - q * h) % 128, 1)
                b = pltpu.roll(right, (at - q * h) % 128, 1)
                edge = jnp.where(lane >= 112, a, b)
                if wide:
                    buf[H - h + q, :, 128:256] = edge
                else:
                    buf[H - h + q] = jnp.where(lane < sz, buf[H - h + q], edge)

    sixth = jnp.float32(1.0 / 6.0)

    def masks(rows, lanes):
        even = (
            lax.broadcasted_iota(jnp.int32, (rows, lanes), 0)
            + lax.broadcasted_iota(jnp.int32, (rows, lanes), 1)
        ) % 2 == 0
        return even, jnp.logical_not(even)

    def beside(a, p, c):
        rows, lanes = c.shape
        t = a[p - 1] + a[p + 1]
        t = t + (pltpu.roll(c, 1, 0) + pltpu.roll(c, rows - 1, 0))
        return t + (pltpu.roll(c, 1, 1) + pltpu.roll(c, lanes - 1, 1))

    def half(a, b, s, lo, hi, H, off, colour, mask, shift=None):
        for p in range(lo, hi):
            c = a[p]
            t = beside(a, p, c) - s[p + off]
            if shift is not None:
                t = t + shift
            b[p] = jnp.where(mask[(p - H + colour) % 2], t * sixth, c)

    fine_mask = masks(Y + 2 * R, 2 * Z)
    one_mask = masks(y1 + 2 * R, 128)

    exchange([(pa, 5, 5, (X, Y, Z), pk_p, rk_p), (den, 4, 5, (X, Y, Z), pk_d, rk_d)])
    for k, (a, b) in enumerate(((pa, pb), (pb, pa), (pa, pb), (pb, pa))):
        d = 4 - k
        half(a, b, den, 5 - d, 5 + X + d, 5, 0, k % 2, fine_mask)
    pairs = []
    total = jnp.zeros((Y, Z), jnp.float32)
    for q in range(x1):
        both = None
        for p in (5 + 2 * q, 6 + 2 * q):
            c = pa[p]
            left = (den[p] - (beside(pa, p, c) - 6.0 * c))[R : R + Y, 0:Z]
            both = left if both is None else both + left
            total = total + den[p, R : R + Y, 0:Z]
            f2[p - 1, R : R + Y, 0:Z] = c[R : R + Y, 0:Z]
        pairs.append(both)
    stacked = jnp.concatenate(pairs, axis=0)
    stacked = jnp.dot(stacked, sz_ref[...], precision=HI, preferred_element_type=jnp.float32)
    one = jnp.dot(sy_ref[...], stacked, precision=HI, preferred_element_type=jnp.float32) * 0.5
    for q in range(x1):
        lv[6 + q, R : R + y1, :] = one[q * y1 : (q + 1) * y1]

    exchange([(lv, 5, 6, (x1, y1, z1), pk_l, rk_l)])
    for p in range(6 - 4, 6 + x1 + 4):
        ea[p] = jnp.where(one_mask[p % 2], lv[p] * -sixth, 0.0)
    for k, (a, b) in enumerate(((ea, eb), (eb, ea), (ea, eb))):
        d = 3 - k
        half(a, b, lv, 6 - d, 6 + x1 + d, 6, 0, (k + 1) % 2, one_mask)
    acc = jnp.zeros((y1, 128), jnp.float32)
    for p in range(6, 6 + x1):
        c = eb[p]
        e2[p, R : R + y1, :] = c[R : R + y1]
        acc = acc + (lv[p] - (beside(eb, p, c) - 6.0 * c))[R : R + y1]
    lane = lax.broadcasted_iota(jnp.int32, (y1, 128), 1)
    acc = jnp.where(lane < z1, acc, 0.0)

    def whole_sum(v):
        return jnp.sum(jnp.sum(v, axis=0, keepdims=True), axis=1, keepdims=True)

    gat[me, :, 0:128] = jnp.broadcast_to(whole_sum(acc), (1, 128))
    gat[me, :, 128:256] = jnp.broadcast_to(whole_sum(total), (1, 128))

    def spread(o, carry):
        pltpu.make_async_remote_copy(
            src_ref=gat.at[me], dst_ref=gat.at[me], send_sem=gs, recv_sem=gr,
            device_id=device(o), device_id_type=MESH,
        ).start()
        return carry

    lax.fori_loop(1, n, spread, 0)
    exchange([(e2, 6, 6, (x1, y1, z1), pk_e, rk_e), (f2, 4, 4, (X, Y, Z), pk_f, rk_f)])
    others = gat.at[pl.ds(0, n - 1)]
    pltpu.make_async_copy(others, others, gs).wait()
    pltpu.make_async_copy(others, others, gr).wait()

    values = gat[:, 0, :]
    blocks = values[:, 0:128]
    mean = jnp.sum(values[:, 128:256], axis=0, keepdims=True) / jnp.float32(n * X * Y * Z)
    blocks = blocks - jnp.sum(blocks, axis=0, keepdims=True) / jnp.float32(n)
    cv[...] = jnp.dot(op_ref[...], blocks, precision=HI, preferred_element_type=jnp.float32)
    row = lax.broadcasted_iota(jnp.int32, (y1 + 2 * R, 128), 0)
    lane = lax.broadcasted_iota(jnp.int32, (y1 + 2 * R, 128), 1)
    maps = []
    for dx in (-1, 0, 1):
        by_row = []
        for dy in (-1, 0, 1):
            vals = []
            for dz in (-1, 0, 1):
                at = (lax.rem(ix + dx + nx, nx) * ny + lax.rem(iy + dy + ny, ny)) * nz
                vals.append(cv[pl.ds(at + lax.rem(iz + dz + nz, nz), 1), :])
            by_row.append(jnp.where(lane < z1, vals[1], jnp.where(lane < (z1 + 128) // 2, vals[2], vals[0])))
        maps.append(jnp.where(row < R, by_row[0], jnp.where(row < R + y1, by_row[1], by_row[2])))
    for p in range(0, x1 + 12):
        which = 0 if p < 6 else (1 if p < 6 + x1 else 2)
        ea[p] = e2[p] + (maps[which] + mean * jnp.float32(8.0 / 3.0))
    for k, (a, b) in enumerate(((ea, eb), (eb, ea), (ea, eb), (eb, ea))):
        d = 5 - k
        half(a, b, lv, 6 - d, 6 + x1 + d, 6, 0, k % 2, one_mask, 4.0 * mean)

    mean2 = jnp.concatenate([mean, mean], axis=1)
    for q in range(4, 6 + x1 + 2):
        wide = jnp.dot(ea[q], rz_ref[...], precision=HI, preferred_element_type=jnp.float32)
        wide = jnp.dot(ry_ref[...], wide, precision=HI, preferred_element_type=jnp.float32)
        wide = wide + mean2 * jnp.float32(2.0 / 3.0)
        for p in (2 * (q - 4), 2 * (q - 4) + 1):
            pb[p] = f2[p] + wide
    for k, (a, b) in enumerate(((pb, pa), (pa, pb), (pb, pa))):
        d = 3 - k
        half(a, b, den, 4 - d, 4 + X + d, 4, 1, k % 2, fine_mask, mean2)
    for p in range(4, 4 + X):
        c = pa[p]
        t = (beside(pa, p, c) - den[p + 1] + mean2) * sixth
        out_ref[p - 4] = jnp.where(fine_mask[(p - 3) % 2], t, c)[R : R + Y, 0:Z]


def body(dims, density, potential):
    nx, ny, nz, X, Y, Z = dims
    n = nx * ny * nz
    x1, y1, z1 = X // 2, Y // 2, Z // 2
    op = coarse_operator(nx, ny, nz, float(y1 * z1), float(x1 * z1), float(x1 * y1))
    sz = (np.arange(Z)[:, None] // 2 == np.arange(128)[None, :]).astype(np.float32)
    r = np.arange(x1 * y1)
    c = np.arange(x1 * Y)
    sy = (r[:, None] == c[None, :] // 2).astype(np.float32)
    rz = (np.arange(128)[:, None] == np.arange(2 * Z)[None, :] // 2).astype(np.float32)
    rows, rows1 = Y + 2 * R, y1 + 2 * R
    ry = (np.arange(rows)[:, None] // 2 + R // 2 == np.arange(rows1)[None, :]).astype(np.float32)
    f32 = jnp.float32
    fine, one = (rows, 128), (rows1, 128)
    vmem = pl.BlockSpec(memory_space=pltpu.VMEM)
    return pl.pallas_call(
        functools.partial(kernel, dims),
        out_shape=jax.ShapeDtypeStruct((X, Y, Z), f32),
        in_specs=[pl.BlockSpec(memory_space=pl.ANY)] * 2 + [vmem] * 5,
        out_specs=vmem,
        scratch_shapes=[
            pltpu.VMEM((X + 10, rows, 2 * Z), f32),
            pltpu.VMEM((X + 10, rows, 2 * Z), f32),
            pltpu.VMEM((X + 10, rows, 2 * Z), f32),
            pltpu.VMEM((x1 + 12, rows1, 128), f32),
            pltpu.VMEM((x1 + 12, rows1, 128), f32),
            pltpu.VMEM((x1 + 12, rows1, 128), f32),
            pltpu.VMEM((x1 + 12, rows1, 128), f32),
            pltpu.VMEM((X + 8, rows, 2 * Z), f32),
            pltpu.VMEM((n, 1, 256), f32),
            pltpu.VMEM((n, 128), f32),
        ]
        + [pltpu.VMEM((2,) + s, f32) for s in (fine, fine, one, one, fine)] * 2
        + [
            pltpu.SemaphoreType.DMA((40,)),
            pltpu.SemaphoreType.DMA((40,)),
            pltpu.SemaphoreType.DMA,
            pltpu.SemaphoreType.DMA,
            pltpu.SemaphoreType.DMA((2,)),
        ],
        compiler_params=pltpu.CompilerParams(collective_id=0, has_side_effects=True),
        name="vcycle",
    )(density, potential, op, sz, sy, rz, ry)


def solution(mesh):
    nx, ny, nz = (mesh.shape[a] for a in ("gx", "gy", "gz"))

    def run(density, potential):
        return body((nx, ny, nz) + density.shape, density, potential)

    spec = P("gx", "gy", "gz")
    return jax.shard_map(run, mesh=mesh, in_specs=(spec, spec), out_specs=spec, check_vma=False)
```

```python
import functools
import numpy as np
import jax
import jax.numpy as jnp
from jax import lax
from jax.experimental import pallas as pl
from jax.experimental.pallas import tpu as pltpu
from jax.sharding import PartitionSpec as P

SWEEPS = 2
HI = lax.Precision.HIGHEST
MESH = pl.DeviceIdType.MESH
R = 8


def table(count):
    modes = (np.arange(count) + 1) // 2
    angle = 2 * np.pi * np.outer(np.arange(count), modes) / count
    q = np.where(np.arange(count) % 2 == 1, np.cos(angle), np.sin(angle)) * np.sqrt(2 / count)
    q = np.where(2 * modes == count, np.cos(angle) / np.sqrt(count), q)
    q[:, 0] = 1 / np.sqrt(count)
    return q, 2 - 2 * np.cos(2 * np.pi * modes / count)


def coarse_operator(nx, ny, nz, wx, wy, wz):
    qx, lx = table(nx)
    qy, ly = table(ny)
    qz, lz = table(nz)
    q = np.kron(np.kron(qx, qy), qz)
    lam = wx * lx[:, None, None] + wy * ly[None, :, None] + wz * lz[None, None, :]
    lam = lam.reshape(-1)
    inv = np.concatenate([[0.0], -1.0 / lam[1:]])
    return ((q * inv) @ q.T).astype(np.float32)


def kernel(
    dims, den_hbm, pot_hbm, op_ref, sz_ref, sy_ref, rz_ref, ry_ref, out_ref,
    own, pm, pa, pb, den, lv, ea, eb, e2, f2, gat, cv,
    pk_p, pk_l, pk_e, pk_f, rk_p, rk_l, rk_e, rk_f,
    ssem, rsem, gs, gr, lsem,
):
    nx, ny, nz, X, Y, Z = dims
    n = nx * ny * nz
    x1, y1, z1 = X // 2, Y // 2, Z // 2
    ix, iy, iz = lax.axis_index("gx"), lax.axis_index("gy"), lax.axis_index("gz")
    me = (ix * ny + iy) * nz + iz

    def device(o):
        ox, oy, oz = o // (ny * nz), (o // nz) % ny, o % nz
        return (lax.rem(ix + ox, nx), lax.rem(iy + oy, ny), lax.rem(iz + oz, nz))

    load_p = pltpu.make_async_copy(pot_hbm, own, lsem.at[0])
    load_d = pltpu.make_async_copy(den_hbm, den.at[pl.ds(6, X), pl.ds(R, Y), pl.ds(0, Z)], lsem.at[1])
    load_p.start()
    load_d.start()

    barrier = pltpu.get_barrier_semaphore()

    def greet(o, carry):
        pl.semaphore_signal(barrier, inc=1, device_id=device(o), device_id_type=MESH)
        return carry

    lax.fori_loop(1, n, greet, 0)
    load_p.wait()
    load_d.wait()
    odd = (
        lax.broadcasted_iota(jnp.int32, (Y, Z), 0) + lax.broadcasted_iota(jnp.int32, (Y, Z), 1)
    ) % 2 == 1
    for j in range(X // 2):
        pm[3 + j, R : R + Y, 0:Z] = jnp.where(odd, own[2 * j], own[2 * j + 1])

    sems = iter(range(200))

    def pack(items, pk):
        base = 0
        sy = items[0][3][1]
        lane = lax.broadcasted_iota(jnp.int32, (sy, 128), 1)
        head = tail = jnp.zeros((sy, 128), jnp.float32)
        for buf, h, H, (sx, sy, sz), deep in items:
            for q in range(sx):
                v = buf[H + q, R : R + sy, 0:128]
                at = base + q * deep
                inside = (lane >= at) & (lane < at + deep)
                tail = jnp.where(inside, pltpu.roll(v, (at - (sz - deep)) % 128, 1), tail)
                head = jnp.where(inside, pltpu.roll(v, at, 1) if at else v, head)
            base += sx * deep
        assert base <= 128
        pk[0] = tail
        pk[1] = head

    def exchange(items, pk, rk):
        copies = []

        def send(src, dst, dx, dy, dz):
            k = next(sems)
            to = (lax.rem(ix + dx + nx, nx), lax.rem(iy + dy + ny, ny), lax.rem(iz + dz + nz, nz))
            copy = pltpu.make_async_remote_copy(
                src_ref=src, dst_ref=dst, send_sem=ssem.at[k], recv_sem=rsem.at[k],
                device_id=to, device_id_type=MESH,
            )
            copy.start()
            copies.append(copy)

        sy = items[0][3][1]
        rows_from = {0: pl.ds(R, sy), 1: pl.ds(sy, R), -1: pl.ds(R, R)}
        rows_to = {0: pl.ds(R, sy), 1: pl.ds(0, R), -1: pl.ds(R + sy, R)}
        for dx in (1, -1, 0):
            for dy in (1, -1, 0):
                for dz in (1, -1):
                    if dx == -1 and nx == 2:
                        continue
                    side = 0 if dz == 1 else 1
                    count = R if dy else sy
                    first = sy - R if dy == 1 else 0
                    send(
                        pk.at[side, pl.ds(first, count)],
                        rk.at[side, 1 - dx, 1 - dy, pl.ds(0, count)],
                        dx, dy, dz,
                    )
                if dx == 0 and dy == 0:
                    continue
                for buf, h, H, (sx, sy, sz), deep in items:
                    p_from = {0: pl.ds(H, sx), 1: pl.ds(H + sx - h, h), -1: pl.ds(H, h)}[dx]
                    p_to = {0: pl.ds(H, sx), 1: pl.ds(H - h, h), -1: pl.ds(H + sx, h)}[dx]
                    lanes = pl.ds(0, 128)
                    send(buf.at[p_from, rows_from[dy], lanes], buf.at[p_to, rows_to[dy], lanes], dx, dy, 0)
        return functools.partial(finish, items, rk, copies)

    def finish(items, rk, copies):
        for copy in copies:
            copy.wait()
        received = {}
        for group in range(3):
            slot = 0 if nx == 2 and group == 2 else group
            for side in range(2):
                received[side, group] = jnp.concatenate(
                    [rk[side, slot, 0, 0:R], rk[side, slot, 1], rk[side, slot, 2, 0:R]], axis=0
                )
        base = 0
        for buf, h, H, (sx, sy, sz), deep in items:
            rows = sy + 2 * R
            lane = lax.broadcasted_iota(jnp.int32, (rows, 128), 1)
            wide = sz == 128
            put = 0 if wide else sz
            for j in range(sx + 2 * h):
                group, q = (0, sx - h + j) if j < h else ((1, j - h) if j < h + sx else (2, j - h - sx))
                at = base + q * deep
                edge = jnp.where(
                    lane >= 112,
                    pltpu.roll(received[0, group], (128 - deep - at) % 128, 1),
                    pltpu.roll(received[1, group], (put - at) % 128, 1),
                )
                if wide:
                    buf[H - h + j, :, 128:256] = edge
                else:
                    buf[H - h + j] = jnp.where(lane < sz, buf[H - h + j], edge)
            base += sx * deep

    sixth = jnp.float32(1.0 / 6.0)

    def masks(rows, lanes):
        even = (
            lax.broadcasted_iota(jnp.int32, (rows, lanes), 0)
            + lax.broadcasted_iota(jnp.int32, (rows, lanes), 1)
        ) % 2 == 0
        return even, jnp.logical_not(even)

    def beside(a, p, c, index=lambda p: p):
        rows, lanes = c.shape
        t = a[index(p - 1)] + a[index(p + 1)]
        t = t + (pltpu.roll(c, 1, 0) + pltpu.roll(c, rows - 1, 0))
        return t + (pltpu.roll(c, 1, 1) + pltpu.roll(c, lanes - 1, 1))

    def half(a, b, s, lo, hi, H, off, colour, mask, shift=None, index=lambda p: p):
        for p in range(lo, hi):
            c = a[index(p)]
            t = beside(a, p, c, index) - s[p + off]
            if shift is not None:
                t = t + shift
            b[p] = jnp.where(mask[(p - H + colour) % 2], t * sixth, c)

    fine_mask = masks(Y + 2 * R, 2 * Z)
    one_mask = masks(y1 + 2 * R, 128)

    first = [(pm, 3, 3, (X // 2, Y, Z), 5), (den, 4, 6, (X, Y, Z), 4)]
    pack(first, pk_p)
    pl.semaphore_wait(barrier, n - 1)
    exchange(first, pk_p, rk_p)()
    for k, (a, b) in enumerate(((pm, pb), (pb, pa), (pa, pb), (pb, pa))):
        d = 4 - k
        index = (lambda p: p // 2) if k == 0 else (lambda p: p)
        half(a, b, den, 6 - d, 6 + X + d, 6, 0, k % 2, fine_mask, None, index)
    pairs = []
    total = jnp.zeros((Y, Z), jnp.float32)
    for q in range(x1):
        both = None
        for p in (6 + 2 * q, 7 + 2 * q):
            c = pa[p]
            left = (den[p] - (beside(pa, p, c) - 6.0 * c))[R : R + Y, 0:Z]
            both = left if both is None else both + left
            total = total + den[p, R : R + Y, 0:Z]
        f2[2 + q, R : R + Y, 0:Z] = jnp.where(
            odd, pa[6 + 2 * q, R : R + Y, 0:Z], pa[7 + 2 * q, R : R + Y, 0:Z]
        )
        pairs.append(both)
    stacked = jnp.concatenate(pairs, axis=0)
    stacked = jnp.dot(stacked, sz_ref[...], precision=HI, preferred_element_type=jnp.float32)
    one = jnp.dot(sy_ref[...], stacked, precision=HI, preferred_element_type=jnp.float32) * 0.5
    for q in range(x1):
        lv[6 + q, R : R + y1, :] = one[q * y1 : (q + 1) * y1]

    second = [(lv, 5, 6, (x1, y1, z1), 5)]
    pack(second, pk_l)
    exchange(second, pk_l, rk_l)()
    for p in range(6 - 4, 6 + x1 + 4):
        ea[p] = jnp.where(one_mask[p % 2], lv[p] * -sixth, 0.0)
    for k, (a, b) in enumerate(((ea, eb), (eb, ea), (ea, eb))):
        d = 3 - k
        half(a, b, lv, 6 - d, 6 + x1 + d, 6, 0, (k + 1) % 2, one_mask)
    acc = jnp.zeros((y1, 128), jnp.float32)
    for p in range(6, 6 + x1):
        c = eb[p]
        acc = acc + (lv[p] - (beside(eb, p, c) - 6.0 * c))[R : R + y1]
    for j in range(x1 // 2):
        e2[3 + j, R : R + y1, :] = jnp.where(
            odd[0:y1], eb[6 + 2 * j, R : R + y1], eb[7 + 2 * j, R : R + y1]
        )
    lane = lax.broadcasted_iota(jnp.int32, (y1, 128), 1)
    acc = jnp.where(lane < z1, acc, 0.0)

    def whole_sum(v):
        return jnp.sum(jnp.sum(v, axis=0, keepdims=True), axis=1, keepdims=True)

    gat[me, :, 0:128] = jnp.broadcast_to(whole_sum(acc), (1, 128))
    gat[me, :, 128:256] = jnp.broadcast_to(whole_sum(total), (1, 128))

    def spread(o, carry):
        pltpu.make_async_remote_copy(
            src_ref=gat.at[me], dst_ref=gat.at[me], send_sem=gs, recv_sem=gr,
            device_id=device(o), device_id_type=MESH,
        ).start()
        return carry

    lax.fori_loop(1, n, spread, 0)
    third = [(e2, 3, 3, (x1 // 2, y1, z1), 6)]
    fourth = [(f2, 2, 2, (X // 2, Y, Z), 4)]
    pack(third, pk_e)
    pack(fourth, pk_f)
    finish_third = exchange(third, pk_e, rk_e)
    finish_fourth = exchange(fourth, pk_f, rk_f)
    finish_third()
    finish_fourth()
    others = gat.at[pl.ds(0, n - 1)]
    pltpu.make_async_copy(others, others, gs).wait()
    pltpu.make_async_copy(others, others, gr).wait()

    values = gat[:, 0, :]
    blocks = values[:, 0:128]
    mean = jnp.sum(values[:, 128:256], axis=0, keepdims=True) / jnp.float32(n * X * Y * Z)
    blocks = blocks - jnp.sum(blocks, axis=0, keepdims=True) / jnp.float32(n)
    cv[...] = jnp.dot(op_ref[...], blocks, precision=HI, preferred_element_type=jnp.float32)
    row = lax.broadcasted_iota(jnp.int32, (y1 + 2 * R, 128), 0)
    lane = lax.broadcasted_iota(jnp.int32, (y1 + 2 * R, 128), 1)
    maps = []
    for dx in (-1, 0, 1):
        by_row = []
        for dy in (-1, 0, 1):
            vals = []
            for dz in (-1, 0, 1):
                at = (lax.rem(ix + dx + nx, nx) * ny + lax.rem(iy + dy + ny, ny)) * nz
                vals.append(cv[pl.ds(at + lax.rem(iz + dz + nz, nz), 1), :])
            by_row.append(jnp.where(lane < z1, vals[1], jnp.where(lane < (z1 + 128) // 2, vals[2], vals[0])))
        maps.append(jnp.where(row < R, by_row[0], jnp.where(row < R + y1, by_row[1], by_row[2])))
    for p in range(0, x1 + 12):
        which = 0 if p < 6 else (1 if p < 6 + x1 else 2)
        ea[p] = e2[p // 2] + (maps[which] + mean * jnp.float32(8.0 / 3.0))
    for k, (a, b) in enumerate(((ea, eb), (eb, ea), (ea, eb), (eb, ea))):
        d = 5 - k
        half(a, b, lv, 6 - d, 6 + x1 + d, 6, 0, k % 2, one_mask, 4.0 * mean)

    mean2 = jnp.concatenate([mean, mean], axis=1)
    for q in range(4, 6 + x1 + 2):
        wide = jnp.dot(ea[q], rz_ref[...], precision=HI, preferred_element_type=jnp.float32)
        wide = jnp.dot(ry_ref[...], wide, precision=HI, preferred_element_type=jnp.float32)
        wide = wide + mean2 * jnp.float32(2.0 / 3.0)
        for p in (2 * (q - 4), 2 * (q - 4) + 1):
            pb[p] = f2[p // 2] + wide
    for k, (a, b) in enumerate(((pb, pa), (pa, pb), (pb, pa))):
        d = 3 - k
        half(a, b, den, 4 - d, 4 + X + d, 4, 2, k % 2, fine_mask, mean2)
    for p in range(4, 4 + X):
        c = pa[p]
        t = (beside(pa, p, c) - den[p + 2] + mean2) * sixth
        out_ref[p - 4] = jnp.where(fine_mask[(p - 3) % 2], t, c)[R : R + Y, 0:Z]


def body(dims, density, potential):
    nx, ny, nz, X, Y, Z = dims
    n = nx * ny * nz
    x1, y1, z1 = X // 2, Y // 2, Z // 2
    op = coarse_operator(nx, ny, nz, float(y1 * z1), float(x1 * z1), float(x1 * y1))
    sz = (np.arange(Z)[:, None] // 2 == np.arange(128)[None, :]).astype(np.float32)
    r = np.arange(x1 * y1)
    c = np.arange(x1 * Y)
    sy = (r[:, None] == c[None, :] // 2).astype(np.float32)
    rz = (np.arange(128)[:, None] == np.arange(2 * Z)[None, :] // 2).astype(np.float32)
    rows, rows1 = Y + 2 * R, y1 + 2 * R
    ry = (np.arange(rows)[:, None] // 2 + R // 2 == np.arange(rows1)[None, :]).astype(np.float32)
    f32 = jnp.float32
    fine, one = (Y, 128), (y1, 128)
    vmem = pl.BlockSpec(memory_space=pltpu.VMEM)
    return pl.pallas_call(
        functools.partial(kernel, dims),
        out_shape=jax.ShapeDtypeStruct((X, Y, Z), f32),
        in_specs=[pl.BlockSpec(memory_space=pl.ANY)] * 2 + [vmem] * 5,
        out_specs=vmem,
        scratch_shapes=[
            pltpu.VMEM((X, Y, Z), f32),
            pltpu.VMEM((X // 2 + 6, rows, 2 * Z), f32),
            pltpu.VMEM((X + 12, rows, 2 * Z), f32),
            pltpu.VMEM((X + 12, rows, 2 * Z), f32),
            pltpu.VMEM((X + 12, rows, 2 * Z), f32),
            pltpu.VMEM((x1 + 12, rows1, 128), f32),
            pltpu.VMEM((x1 + 12, rows1, 128), f32),
            pltpu.VMEM((x1 + 12, rows1, 128), f32),
            pltpu.VMEM((x1 // 2 + 6, rows1, 128), f32),
            pltpu.VMEM((X // 2 + 4, rows, 2 * Z), f32),
            pltpu.VMEM((n, 1, 256), f32),
            pltpu.VMEM((n, 128), f32),
        ]
        + [pltpu.VMEM(lead + s, f32) for lead in ((2,), (2, 3, 3)) for s in (fine, one, one, fine)]
        + [
            pltpu.SemaphoreType.DMA((120,)),
            pltpu.SemaphoreType.DMA((120,)),
            pltpu.SemaphoreType.DMA,
            pltpu.SemaphoreType.DMA,
            pltpu.SemaphoreType.DMA((2,)),
        ],
        compiler_params=pltpu.CompilerParams(collective_id=0, has_side_effects=True),
        name="vcycle",
    )(density, potential, op, sz, sy, rz, ry)


def solution(mesh):
    nx, ny, nz = (mesh.shape[a] for a in ("gx", "gy", "gz"))

    def run(density, potential):
        return body((nx, ny, nz) + density.shape, density, potential)

    spec = P("gx", "gy", "gz")
    return jax.shard_map(run, mesh=mesh, in_specs=(spec, spec), out_specs=spec, check_vma=False)
```

```python
import functools
import numpy as np
import jax
import jax.numpy as jnp
from jax import lax
from jax.experimental import pallas as pl
from jax.experimental.pallas import tpu as pltpu
from jax.sharding import PartitionSpec as P

SWEEPS = 2
HI = lax.Precision.HIGHEST
MESH = pl.DeviceIdType.MESH
R = 8


def table(count):
    modes = (np.arange(count) + 1) // 2
    angle = 2 * np.pi * np.outer(np.arange(count), modes) / count
    q = np.where(np.arange(count) % 2 == 1, np.cos(angle), np.sin(angle)) * np.sqrt(2 / count)
    q = np.where(2 * modes == count, np.cos(angle) / np.sqrt(count), q)
    q[:, 0] = 1 / np.sqrt(count)
    return q, 2 - 2 * np.cos(2 * np.pi * modes / count)


def coarse_operator(nx, ny, nz, wx, wy, wz):
    qx, lx = table(nx)
    qy, ly = table(ny)
    qz, lz = table(nz)
    q = np.kron(np.kron(qx, qy), qz)
    lam = wx * lx[:, None, None] + wy * ly[None, :, None] + wz * lz[None, None, :]
    lam = lam.reshape(-1)
    inv = np.concatenate([[0.0], -1.0 / lam[1:]])
    return ((q * inv) @ q.T).astype(np.float32)


def kernel(
    dims, den_hbm, pot_hbm, op_hbm, out_ref, op_ref,
    own, pm, pa, pb, den, lv, ea, eb, e2, f2, gat, cv,
    pk_p, pk_l, pk_e, pk_f, rk_p, rk_l, rk_e, rk_f,
    ssem, rsem, gs, gr, lsem,
):
    nx, ny, nz, X, Y, Z = dims
    n = nx * ny * nz
    x1, y1, z1 = X // 2, Y // 2, Z // 2
    ix, iy, iz = lax.axis_index("gx"), lax.axis_index("gy"), lax.axis_index("gz")
    me = (ix * ny + iy) * nz + iz

    def around(i, count):
        return [i] + [jnp.where(i + o >= count, i + o - count, i + o) for o in range(1, count)]

    xs, ys, zs = around(ix, nx), around(iy, ny), around(iz, nz)

    def device(o):
        if isinstance(o, int):
            return (xs[o // (ny * nz)], ys[o // nz % ny], zs[o % nz])
        ox, oy, oz = o // (ny * nz), (o // nz) % ny, o % nz
        return (lax.rem(ix + ox, nx), lax.rem(iy + oy, ny), lax.rem(iz + oz, nz))

    def each_other(step):
        if n <= 64:
            for o in range(1, n):
                step(o, 0)
        else:
            lax.fori_loop(1, n, step, 0)

    load_p = pltpu.make_async_copy(pot_hbm, own, lsem.at[0])
    load_d = pltpu.make_async_copy(den_hbm, den.at[pl.ds(6, X), pl.ds(R, Y), pl.ds(0, Z)], lsem.at[1])
    load_p.start()
    load_d.start()
    load_op = pltpu.make_async_copy(op_hbm, op_ref, lsem.at[2])
    load_op.start()

    barrier = pltpu.get_barrier_semaphore()

    def greet(o, carry):
        pl.semaphore_signal(barrier, inc=1, device_id=device(o), device_id_type=MESH)
        return carry

    each_other(greet)
    load_p.wait()
    load_d.wait()
    odd = (
        lax.broadcasted_iota(jnp.int32, (Y, Z), 0) + lax.broadcasted_iota(jnp.int32, (Y, Z), 1)
    ) % 2 == 1
    for j in range(X // 2):
        pm[3 + j, R : R + Y, 0:Z] = jnp.where(odd, own[2 * j], own[2 * j + 1])

    sems = iter(range(200))

    def pack(items, pk):
        base = 0
        sy = items[0][3][1]
        lane = lax.broadcasted_iota(jnp.int32, (sy, 128), 1)
        head = tail = jnp.zeros((sy, 128), jnp.float32)
        for buf, h, H, (sx, sy, sz), deep in items:
            for q in range(sx):
                v = buf[H + q, R : R + sy, 0:128]
                at = base + q * deep
                inside = (lane >= at) & (lane < at + deep)
                tail = jnp.where(inside, pltpu.roll(v, (at - (sz - deep)) % 128, 1), tail)
                head = jnp.where(inside, pltpu.roll(v, at, 1) if at else v, head)
            base += sx * deep
        assert base <= 128
        pk[0] = tail
        pk[1] = head

    def exchange(items, pk, rk):
        copies = []

        def send(src, dst, dx, dy, dz):
            k = next(sems)
            to = (xs[dx], ys[dy], zs[dz])
            copy = pltpu.make_async_remote_copy(
                src_ref=src, dst_ref=dst, send_sem=ssem.at[k], recv_sem=rsem.at[k],
                device_id=to, device_id_type=MESH,
            )
            copy.start()
            copies.append(copy)

        sy = items[0][3][1]
        rows_from = {0: pl.ds(R, sy), 1: pl.ds(sy, R), -1: pl.ds(R, R)}
        rows_to = {0: pl.ds(R, sy), 1: pl.ds(0, R), -1: pl.ds(R + sy, R)}
        for dx in (1, -1, 0):
            for dy in (1, -1, 0):
                for dz in (1, -1):
                    if dx == -1 and nx == 2:
                        continue
                    side = 0 if dz == 1 else 1
                    count = R if dy else sy
                    first = sy - R if dy == 1 else 0
                    send(
                        pk.at[side, pl.ds(first, count)],
                        rk.at[side, 1 - dx, 1 - dy, pl.ds(0, count)],
                        dx, dy, dz,
                    )
                if dx == 0 and dy == 0:
                    continue
                for buf, h, H, (sx, sy, sz), deep in items:
                    p_from = {0: pl.ds(H, sx), 1: pl.ds(H + sx - h, h), -1: pl.ds(H, h)}[dx]
                    p_to = {0: pl.ds(H, sx), 1: pl.ds(H - h, h), -1: pl.ds(H + sx, h)}[dx]
                    lanes = pl.ds(0, 128)
                    send(buf.at[p_from, rows_from[dy], lanes], buf.at[p_to, rows_to[dy], lanes], dx, dy, 0)
        return functools.partial(finish, items, rk, copies)

    def finish(items, rk, copies):
        for copy in copies:
            copy.wait()
        received = {}
        for group in range(3):
            slot = 0 if nx == 2 and group == 2 else group
            for side in range(2):
                received[side, group] = jnp.concatenate(
                    [rk[side, slot, 0, 0:R], rk[side, slot, 1], rk[side, slot, 2, 0:R]], axis=0
                )
        base = 0
        for buf, h, H, (sx, sy, sz), deep in items:
            rows = sy + 2 * R
            lane = lax.broadcasted_iota(jnp.int32, (rows, 128), 1)
            wide = sz == 128
            put = 0 if wide else sz
            for j in range(sx + 2 * h):
                group, q = (0, sx - h + j) if j < h else ((1, j - h) if j < h + sx else (2, j - h - sx))
                at = base + q * deep
                edge = jnp.where(
                    lane >= 112,
                    pltpu.roll(received[0, group], (128 - deep - at) % 128, 1),
                    pltpu.roll(received[1, group], (put - at) % 128, 1),
                )
                if wide:
                    buf[H - h + j, :, 128:256] = edge
                else:
                    buf[H - h + j] = jnp.where(lane < sz, buf[H - h + j], edge)
            base += sx * deep

    sixth = jnp.float32(1.0 / 6.0)

    def masks(rows, lanes):
        even = (
            lax.broadcasted_iota(jnp.int32, (rows, lanes), 0)
            + lax.broadcasted_iota(jnp.int32, (rows, lanes), 1)
        ) % 2 == 0
        return even, jnp.logical_not(even)

    def beside(a, p, c, index=lambda p: p):
        rows, lanes = c.shape
        t = a[index(p - 1)] + a[index(p + 1)]
        t = t + (pltpu.roll(c, 1, 0) + pltpu.roll(c, rows - 1, 0))
        return t + (pltpu.roll(c, 1, 1) + pltpu.roll(c, lanes - 1, 1))

    def half(a, b, s, lo, hi, H, off, colour, mask, shift=None, index=lambda p: p):
        for p in range(lo, hi):
            c = a[index(p)]
            t = beside(a, p, c, index) - s[p + off]
            if shift is not None:
                t = t + shift
            b[p] = jnp.where(mask[(p - H + colour) % 2], t * sixth, c)

    fine_mask = masks(Y + 2 * R, 2 * Z)
    one_mask = masks(y1 + 2 * R, 128)

    first = [(pm, 3, 3, (X // 2, Y, Z), 5), (den, 4, 6, (X, Y, Z), 4)]
    pack(first, pk_p)
    pl.semaphore_wait(barrier, n - 1)
    exchange(first, pk_p, rk_p)()
    for k, (a, b) in enumerate(((pm, pb), (pb, pa), (pa, pb), (pb, pa))):
        d = 4 - k
        index = (lambda p: p // 2) if k == 0 else (lambda p: p)
        half(a, b, den, 6 - d, 6 + X + d, 6, 0, k % 2, fine_mask, None, index)
    pairs = []
    total = jnp.zeros((Y, Z), jnp.float32)
    for q in range(x1):
        both = None
        for p in (6 + 2 * q, 7 + 2 * q):
            c = pa[p]
            left = (den[p] - (beside(pa, p, c) - 6.0 * c))[R : R + Y, 0:Z]
            both = left if both is None else both + left
            total = total + den[p, R : R + Y, 0:Z]
        f2[2 + q, R : R + Y, 0:Z] = jnp.where(
            odd, pa[6 + 2 * q, R : R + Y, 0:Z], pa[7 + 2 * q, R : R + Y, 0:Z]
        )
        pairs.append(both)
    def halves(shape, dim, start=0):
        i = [lax.broadcasted_iota(jnp.int32, shape, k) for k in (0, 1)]
        return jnp.where((i[dim] >> 1) + start == i[1 - dim], 1.0, 0.0).astype(jnp.float32)

    to_z, to_y = halves((Z, 128), 0), halves((x1 * y1, x1 * Y), 1)
    from_z, from_y = halves((128, 2 * Z), 1), halves((Y + 2 * R, y1 + 2 * R), 0, R // 2)
    stacked = jnp.concatenate(pairs, axis=0)
    stacked = jnp.dot(stacked, to_z, precision=HI, preferred_element_type=jnp.float32)
    one = jnp.dot(to_y, stacked, precision=HI, preferred_element_type=jnp.float32) * 0.5
    for q in range(x1):
        lv[6 + q, R : R + y1, :] = one[q * y1 : (q + 1) * y1]

    second = [(lv, 5, 6, (x1, y1, z1), 5)]
    pack(second, pk_l)
    exchange(second, pk_l, rk_l)()
    for p in range(6 - 4, 6 + x1 + 4):
        ea[p] = jnp.where(one_mask[p % 2], lv[p] * -sixth, 0.0)
    for k, (a, b) in enumerate(((ea, eb), (eb, ea), (ea, eb))):
        d = 3 - k
        half(a, b, lv, 6 - d, 6 + x1 + d, 6, 0, (k + 1) % 2, one_mask)
    acc = jnp.zeros((y1, 128), jnp.float32)
    for p in range(6, 6 + x1):
        c = eb[p]
        acc = acc + (lv[p] - (beside(eb, p, c) - 6.0 * c))[R : R + y1]
    for j in range(x1 // 2):
        e2[3 + j, R : R + y1, :] = jnp.where(
            odd[0:y1], eb[6 + 2 * j, R : R + y1], eb[7 + 2 * j, R : R + y1]
        )
    lane = lax.broadcasted_iota(jnp.int32, (y1, 128), 1)
    acc = jnp.where(lane < z1, acc, 0.0)

    def whole_sum(v):
        return jnp.sum(jnp.sum(v, axis=0, keepdims=True), axis=1, keepdims=True)

    gat[me, :, 0:128] = jnp.broadcast_to(whole_sum(acc), (1, 128))
    gat[me, :, 128:256] = jnp.broadcast_to(whole_sum(total), (1, 128))

    def spread(o, carry):
        pltpu.make_async_remote_copy(
            src_ref=gat.at[me], dst_ref=gat.at[me], send_sem=gs, recv_sem=gr,
            device_id=device(o), device_id_type=MESH,
        ).start()
        return carry

    each_other(spread)
    third = [(e2, 3, 3, (x1 // 2, y1, z1), 6)]
    fourth = [(f2, 2, 2, (X // 2, Y, Z), 4)]
    pack(third, pk_e)
    pack(fourth, pk_f)
    finish_third = exchange(third, pk_e, rk_e)
    finish_fourth = exchange(fourth, pk_f, rk_f)
    finish_third()
    finish_fourth()
    others = gat.at[pl.ds(0, n - 1)]
    pltpu.make_async_copy(others, others, gs).wait()
    pltpu.make_async_copy(others, others, gr).wait()

    load_op.wait()
    values = gat[:, 0, :]
    blocks = values[:, 0:128]
    mean = jnp.sum(values[:, 128:256], axis=0, keepdims=True) / jnp.float32(n * X * Y * Z)
    blocks = blocks - jnp.sum(blocks, axis=0, keepdims=True) / jnp.float32(n)
    cv[...] = jnp.dot(op_ref[...], blocks, precision=HI, preferred_element_type=jnp.float32)
    row = lax.broadcasted_iota(jnp.int32, (y1 + 2 * R, 128), 0)
    lane = lax.broadcasted_iota(jnp.int32, (y1 + 2 * R, 128), 1)
    maps = []
    for dx in (-1, 0, 1):
        by_row = []
        for dy in (-1, 0, 1):
            vals = []
            for dz in (-1, 0, 1):
                at = (xs[dx] * ny + ys[dy]) * nz
                vals.append(cv[pl.ds(at + zs[dz], 1), :])
            by_row.append(jnp.where(lane < z1, vals[1], jnp.where(lane < (z1 + 128) // 2, vals[2], vals[0])))
        maps.append(jnp.where(row < R, by_row[0], jnp.where(row < R + y1, by_row[1], by_row[2])))
    for p in range(0, x1 + 12):
        which = 0 if p < 6 else (1 if p < 6 + x1 else 2)
        ea[p] = e2[p // 2] + (maps[which] + mean * jnp.float32(8.0 / 3.0))
    for k, (a, b) in enumerate(((ea, eb), (eb, ea), (ea, eb), (eb, ea))):
        d = 5 - k
        half(a, b, lv, 6 - d, 6 + x1 + d, 6, 0, k % 2, one_mask, 4.0 * mean)

    mean2 = jnp.concatenate([mean, mean], axis=1)
    for q in range(4, 6 + x1 + 2):
        wide = jnp.dot(ea[q], from_z, precision=HI, preferred_element_type=jnp.float32)
        wide = jnp.dot(from_y, wide, precision=HI, preferred_element_type=jnp.float32)
        wide = wide + mean2 * jnp.float32(2.0 / 3.0)
        for p in (2 * (q - 4), 2 * (q - 4) + 1):
            pb[p] = f2[p // 2] + wide
    for k, (a, b) in enumerate(((pb, pa), (pa, pb), (pb, pa))):
        d = 3 - k
        half(a, b, den, 4 - d, 4 + X + d, 4, 2, k % 2, fine_mask, mean2)
    for p in range(4, 4 + X):
        c = pa[p]
        t = (beside(pa, p, c) - den[p + 2] + mean2) * sixth
        out_ref[p - 4] = jnp.where(fine_mask[(p - 3) % 2], t, c)[R : R + Y, 0:Z]


def body(dims, density, potential):
    nx, ny, nz, X, Y, Z = dims
    n = nx * ny * nz
    x1, y1, z1 = X // 2, Y // 2, Z // 2
    op = coarse_operator(nx, ny, nz, float(y1 * z1), float(x1 * z1), float(x1 * y1))
    rows, rows1 = Y + 2 * R, y1 + 2 * R
    f32 = jnp.float32
    fine, one = (Y, 128), (y1, 128)
    vmem = pl.BlockSpec(memory_space=pltpu.VMEM)
    return pl.pallas_call(
        functools.partial(kernel, dims),
        out_shape=jax.ShapeDtypeStruct((X, Y, Z), f32),
        in_specs=[pl.BlockSpec(memory_space=pl.ANY)] * 3,
        out_specs=vmem,
        scratch_shapes=[
            pltpu.VMEM((n, n), f32),
            pltpu.VMEM((X, Y, Z), f32),
            pltpu.VMEM((X // 2 + 6, rows, 2 * Z), f32),
            pltpu.VMEM((X + 12, rows, 2 * Z), f32),
            pltpu.VMEM((X + 12, rows, 2 * Z), f32),
            pltpu.VMEM((X + 12, rows, 2 * Z), f32),
            pltpu.VMEM((x1 + 12, rows1, 128), f32),
            pltpu.VMEM((x1 + 12, rows1, 128), f32),
            pltpu.VMEM((x1 + 12, rows1, 128), f32),
            pltpu.VMEM((x1 // 2 + 6, rows1, 128), f32),
            pltpu.VMEM((X // 2 + 4, rows, 2 * Z), f32),
            pltpu.VMEM((n, 1, 256), f32),
            pltpu.VMEM((n, 128), f32),
        ]
        + [pltpu.VMEM(lead + s, f32) for lead in ((2,), (2, 3, 3)) for s in (fine, one, one, fine)]
        + [
            pltpu.SemaphoreType.DMA((120,)),
            pltpu.SemaphoreType.DMA((120,)),
            pltpu.SemaphoreType.DMA,
            pltpu.SemaphoreType.DMA,
            pltpu.SemaphoreType.DMA((3,)),
        ],
        compiler_params=pltpu.CompilerParams(collective_id=0, has_side_effects=True),
        name="vcycle",
    )(density, potential, op)


def solution(mesh):
    nx, ny, nz = (mesh.shape[a] for a in ("gx", "gy", "gz"))

    def run(density, potential):
        return body((nx, ny, nz) + density.shape, density, potential)

    spec = P("gx", "gy", "gz")
    return jax.shard_map(run, mesh=mesh, in_specs=(spec, spec), out_specs=spec, check_vma=False)
```

```python
import functools
import numpy as np
import jax
import jax.numpy as jnp
from jax import lax
from jax.experimental import pallas as pl
from jax.experimental.pallas import tpu as pltpu
from jax.sharding import PartitionSpec as P

SWEEPS = 2
HI = lax.Precision.HIGHEST
MESH = pl.DeviceIdType.MESH
R = 8


def table(count):
    modes = (np.arange(count) + 1) // 2
    angle = 2 * np.pi * np.outer(np.arange(count), modes) / count
    q = np.where(np.arange(count) % 2 == 1, np.cos(angle), np.sin(angle)) * np.sqrt(2 / count)
    q = np.where(2 * modes == count, np.cos(angle) / np.sqrt(count), q)
    q[:, 0] = 1 / np.sqrt(count)
    return q, 2 - 2 * np.cos(2 * np.pi * modes / count)


def coarse_operator(nx, ny, nz, wx, wy, wz):
    qx, lx = table(nx)
    qy, ly = table(ny)
    qz, lz = table(nz)
    q = np.kron(np.kron(qx, qy), qz)
    lam = wx * lx[:, None, None] + wy * ly[None, :, None] + wz * lz[None, None, :]
    lam = lam.reshape(-1)
    inv = np.concatenate([[0.0], -1.0 / lam[1:]])
    return ((q * inv) @ q.T).astype(np.float32)


def kernel(
    dims, den_hbm, pot_hbm, op_hbm, out_ref, op_ref,
    own, pm, pa, pb, den, lv, ea, eb, e2, f2, gat, cv,
    pk_p, pk_l, pk_e, pk_f, rk_p, rk_l, rk_e, rk_f,
    ssem, rsem, gs, gr, lsem,
):
    nx, ny, nz, X, Y, Z = dims
    n = nx * ny * nz
    x1, y1, z1 = X // 2, Y // 2, Z // 2
    ix, iy, iz = lax.axis_index("gx"), lax.axis_index("gy"), lax.axis_index("gz")
    me = (ix * ny + iy) * nz + iz

    def around(i, count):
        return [i] + [jnp.where(i + o >= count, i + o - count, i + o) for o in range(1, count)]

    xs, ys, zs = around(ix, nx), around(iy, ny), around(iz, nz)

    def device(o):
        if isinstance(o, int):
            return (xs[o // (ny * nz)], ys[o // nz % ny], zs[o % nz])
        ox, oy, oz = o // (ny * nz), (o // nz) % ny, o % nz
        return (lax.rem(ix + ox, nx), lax.rem(iy + oy, ny), lax.rem(iz + oz, nz))

    def each_other(step):
        if n <= 64:
            for o in range(1, n):
                step(o, 0)
        else:
            lax.fori_loop(1, n, step, 0)

    load_p = pltpu.make_async_copy(pot_hbm, own, lsem.at[0])
    load_d = pltpu.make_async_copy(den_hbm, den.at[pl.ds(6, X), pl.ds(R, Y), pl.ds(0, Z)], lsem.at[1])
    load_p.start()
    load_d.start()
    load_op = pltpu.make_async_copy(op_hbm, op_ref, lsem.at[2])
    load_op.start()

    barrier = pltpu.get_barrier_semaphore()

    def greet(o, carry):
        pl.semaphore_signal(barrier, inc=1, device_id=device(o), device_id_type=MESH)
        return carry

    near = max(nx, ny, nz) <= 5
    steps = sorted({
        (dx % nx * ny + dy % ny) * nz + dz % nz
        for dx in (-1, 0, 1) for dy in (-1, 0, 1) for dz in (-1, 0, 1)
    } - {0})
    if near:
        for o in steps:
            greet(o, 0)
    else:
        each_other(greet)
    load_p.wait()
    load_d.wait()
    odd = (
        lax.broadcasted_iota(jnp.int32, (Y, Z), 0) + lax.broadcasted_iota(jnp.int32, (Y, Z), 1)
    ) % 2 == 1
    for j in range(X // 2):
        pm[3 + j, R : R + Y, 0:Z] = jnp.where(odd, own[2 * j], own[2 * j + 1])

    sems = iter(range(200))

    def pack(items, pk):
        base = 0
        sy = items[0][3][1]
        lane = lax.broadcasted_iota(jnp.int32, (sy, 128), 1)
        head = tail = jnp.zeros((sy, 128), jnp.float32)
        for buf, h, H, (sx, sy, sz), deep in items:
            for q in range(sx):
                v = buf[H + q, R : R + sy, 0:128]
                at = base + q * deep
                inside = (lane >= at) & (lane < at + deep)
                tail = jnp.where(inside, pltpu.roll(v, (at - (sz - deep)) % 128, 1), tail)
                head = jnp.where(inside, pltpu.roll(v, at, 1) if at else v, head)
            base += sx * deep
        assert base <= 128
        pk[0] = tail
        pk[1] = head

    def exchange(items, pk, rk):
        copies = []

        def send(src, dst, dx, dy, dz):
            k = next(sems)
            to = (xs[dx], ys[dy], zs[dz])
            copy = pltpu.make_async_remote_copy(
                src_ref=src, dst_ref=dst, send_sem=ssem.at[k], recv_sem=rsem.at[k],
                device_id=to, device_id_type=MESH,
            )
            copy.start()
            copies.append(copy)

        sy = items[0][3][1]
        rows_from = {0: pl.ds(R, sy), 1: pl.ds(sy, R), -1: pl.ds(R, R)}
        rows_to = {0: pl.ds(R, sy), 1: pl.ds(0, R), -1: pl.ds(R + sy, R)}
        for dx in (1, -1, 0):
            for dy in (1, -1, 0):
                for dz in (1, -1):
                    if dx == -1 and nx == 2:
                        continue
                    side = 0 if dz == 1 else 1
                    count = R if dy else sy
                    first = sy - R if dy == 1 else 0
                    send(
                        pk.at[side, pl.ds(first, count)],
                        rk.at[side, 1 - dx, 1 - dy, pl.ds(0, count)],
                        dx, dy, dz,
                    )
                if dx == 0 and dy == 0:
                    continue
                for buf, h, H, (sx, sy, sz), deep in items:
                    p_from = {0: pl.ds(H, sx), 1: pl.ds(H + sx - h, h), -1: pl.ds(H, h)}[dx]
                    p_to = {0: pl.ds(H, sx), 1: pl.ds(H - h, h), -1: pl.ds(H + sx, h)}[dx]
                    lanes = pl.ds(0, 128)
                    send(buf.at[p_from, rows_from[dy], lanes], buf.at[p_to, rows_to[dy], lanes], dx, dy, 0)
        return functools.partial(finish, items, rk, copies)

    def finish(items, rk, copies):
        for copy in copies:
            copy.wait()
        received = {}
        for group in range(3):
            slot = 0 if nx == 2 and group == 2 else group
            for side in range(2):
                received[side, group] = jnp.concatenate(
                    [rk[side, slot, 0, 0:R], rk[side, slot, 1], rk[side, slot, 2, 0:R]], axis=0
                )
        base = 0
        for buf, h, H, (sx, sy, sz), deep in items:
            rows = sy + 2 * R
            lane = lax.broadcasted_iota(jnp.int32, (rows, 128), 1)
            wide = sz == 128
            put = 0 if wide else sz
            for j in range(sx + 2 * h):
                group, q = (0, sx - h + j) if j < h else ((1, j - h) if j < h + sx else (2, j - h - sx))
                at = base + q * deep
                edge = jnp.where(
                    lane >= 112,
                    pltpu.roll(received[0, group], (128 - deep - at) % 128, 1),
                    pltpu.roll(received[1, group], (put - at) % 128, 1),
                )
                if wide:
                    buf[H - h + j, :, 128:256] = edge
                else:
                    buf[H - h + j] = jnp.where(lane < sz, buf[H - h + j], edge)
            base += sx * deep

    sixth = jnp.float32(1.0 / 6.0)

    def masks(rows, lanes):
        even = (
            lax.broadcasted_iota(jnp.int32, (rows, lanes), 0)
            + lax.broadcasted_iota(jnp.int32, (rows, lanes), 1)
        ) % 2 == 0
        return even, jnp.logical_not(even)

    def beside(a, p, c, index=lambda p: p):
        rows, lanes = c.shape
        t = a[index(p - 1)] + a[index(p + 1)]
        t = t + (pltpu.roll(c, 1, 0) + pltpu.roll(c, rows - 1, 0))
        return t + (pltpu.roll(c, 1, 1) + pltpu.roll(c, lanes - 1, 1))

    def half(a, b, s, lo, hi, H, off, colour, mask, shift=None, index=lambda p: p):
        for p in range(lo, hi):
            c = a[index(p)]
            t = beside(a, p, c, index) - s[p + off]
            if shift is not None:
                t = t + shift
            b[p] = jnp.where(mask[(p - H + colour) % 2], t * sixth, c)

    fine_mask = masks(Y + 2 * R, 2 * Z)
    one_mask = masks(y1 + 2 * R, 128)

    first = [(pm, 3, 3, (X // 2, Y, Z), 5), (den, 4, 6, (X, Y, Z), 4)]
    pack(first, pk_p)
    pl.semaphore_wait(barrier, len(steps) if near else n - 1)
    exchange(first, pk_p, rk_p)()
    for k, (a, b) in enumerate(((pm, pb), (pb, pa), (pa, pb), (pb, pa))):
        d = 4 - k
        index = (lambda p: p // 2) if k == 0 else (lambda p: p)
        half(a, b, den, 6 - d, 6 + X + d, 6, 0, k % 2, fine_mask, None, index)
    pairs = []
    total = jnp.zeros((Y, Z), jnp.float32)
    for q in range(x1):
        both = None
        for p in (6 + 2 * q, 7 + 2 * q):
            c = pa[p]
            left = (den[p] - (beside(pa, p, c) - 6.0 * c))[R : R + Y, 0:Z]
            both = left if both is None else both + left
            total = total + den[p, R : R + Y, 0:Z]
        f2[2 + q, R : R + Y, 0:Z] = jnp.where(
            odd, pa[6 + 2 * q, R : R + Y, 0:Z], pa[7 + 2 * q, R : R + Y, 0:Z]
        )
        pairs.append(both)
    def halves(shape, dim, start=0):
        i = [lax.broadcasted_iota(jnp.int32, shape, k) for k in (0, 1)]
        return jnp.where((i[dim] >> 1) + start == i[1 - dim], 1.0, 0.0).astype(jnp.float32)

    to_z, to_y = halves((Z, 128), 0), halves((x1 * y1, x1 * Y), 1)
    from_z, from_y = halves((128, 2 * Z), 1), halves((Y + 2 * R, y1 + 2 * R), 0, R // 2)
    stacked = jnp.concatenate(pairs, axis=0)
    stacked = jnp.dot(stacked, to_z, precision=HI, preferred_element_type=jnp.float32)
    one = jnp.dot(to_y, stacked, precision=HI, preferred_element_type=jnp.float32) * 0.5
    for q in range(x1):
        lv[6 + q, R : R + y1, :] = one[q * y1 : (q + 1) * y1]

    second = [(lv, 5, 6, (x1, y1, z1), 5)]
    pack(second, pk_l)
    finish_second = exchange(second, pk_l, rk_l)
    fourth = [(f2, 2, 2, (X // 2, Y, Z), 4)]
    pack(fourth, pk_f)
    finish_fourth = exchange(fourth, pk_f, rk_f)
    finish_second()
    for p in range(6 - 4, 6 + x1 + 4):
        ea[p] = jnp.where(one_mask[p % 2], lv[p] * -sixth, 0.0)
    for k, (a, b) in enumerate(((ea, eb), (eb, ea), (ea, eb))):
        d = 3 - k
        half(a, b, lv, 6 - d, 6 + x1 + d, 6, 0, (k + 1) % 2, one_mask)
    acc = jnp.zeros((y1, 128), jnp.float32)
    for p in range(6, 6 + x1):
        c = eb[p]
        acc = acc + (lv[p] - (beside(eb, p, c) - 6.0 * c))[R : R + y1]
    for j in range(x1 // 2):
        e2[3 + j, R : R + y1, :] = jnp.where(
            odd[0:y1], eb[6 + 2 * j, R : R + y1], eb[7 + 2 * j, R : R + y1]
        )
    lane = lax.broadcasted_iota(jnp.int32, (y1, 128), 1)
    acc = jnp.where(lane < z1, acc, 0.0)

    def whole_sum(v):
        return jnp.sum(jnp.sum(v, axis=0, keepdims=True), axis=1, keepdims=True)

    gat[me, :, 0:128] = jnp.broadcast_to(whole_sum(acc), (1, 128))
    gat[me, :, 128:256] = jnp.broadcast_to(whole_sum(total), (1, 128))

    def spread(o, carry):
        pltpu.make_async_remote_copy(
            src_ref=gat.at[me], dst_ref=gat.at[me], send_sem=gs, recv_sem=gr,
            device_id=device(o), device_id_type=MESH,
        ).start()
        return carry

    each_other(spread)
    third = [(e2, 3, 3, (x1 // 2, y1, z1), 6)]
    pack(third, pk_e)
    finish_third = exchange(third, pk_e, rk_e)
    finish_third()
    finish_fourth()
    others = gat.at[pl.ds(0, n - 1)]
    pltpu.make_async_copy(others, others, gs).wait()
    pltpu.make_async_copy(others, others, gr).wait()

    load_op.wait()
    values = gat[:, 0, :]
    blocks = values[:, 0:128]
    mean = jnp.sum(values[:, 128:256], axis=0, keepdims=True) / jnp.float32(n * X * Y * Z)
    blocks = blocks - jnp.sum(blocks, axis=0, keepdims=True) / jnp.float32(n)
    cv[...] = jnp.dot(op_ref[...], blocks, precision=HI, preferred_element_type=jnp.float32)
    row = lax.broadcasted_iota(jnp.int32, (y1 + 2 * R, 128), 0)
    lane = lax.broadcasted_iota(jnp.int32, (y1 + 2 * R, 128), 1)
    maps = []
    for dx in (-1, 0, 1):
        by_row = []
        for dy in (-1, 0, 1):
            vals = []
            for dz in (-1, 0, 1):
                at = (xs[dx] * ny + ys[dy]) * nz
                vals.append(cv[pl.ds(at + zs[dz], 1), :])
            by_row.append(jnp.where(lane < z1, vals[1], jnp.where(lane < (z1 + 128) // 2, vals[2], vals[0])))
        maps.append(jnp.where(row < R, by_row[0], jnp.where(row < R + y1, by_row[1], by_row[2])))
    for p in range(0, x1 + 12):
        which = 0 if p < 6 else (1 if p < 6 + x1 else 2)
        ea[p] = e2[p // 2] + (maps[which] + mean * jnp.float32(8.0 / 3.0))
    for k, (a, b) in enumerate(((ea, eb), (eb, ea), (ea, eb), (eb, ea))):
        d = 5 - k
        half(a, b, lv, 6 - d, 6 + x1 + d, 6, 0, k % 2, one_mask, 4.0 * mean)

    mean2 = jnp.concatenate([mean, mean], axis=1)
    for q in range(4, 6 + x1 + 2):
        wide = jnp.dot(ea[q], from_z, precision=HI, preferred_element_type=jnp.float32)
        wide = jnp.dot(from_y, wide, precision=HI, preferred_element_type=jnp.float32)
        wide = wide + mean2 * jnp.float32(2.0 / 3.0)
        for p in (2 * (q - 4), 2 * (q - 4) + 1):
            pb[p] = f2[p // 2] + wide
    for k, (a, b) in enumerate(((pb, pa), (pa, pb), (pb, pa))):
        d = 3 - k
        half(a, b, den, 4 - d, 4 + X + d, 4, 2, k % 2, fine_mask, mean2)
    for p in range(4, 4 + X):
        c = pa[p]
        t = (beside(pa, p, c) - den[p + 2] + mean2) * sixth
        out_ref[p - 4] = jnp.where(fine_mask[(p - 3) % 2], t, c)[R : R + Y, 0:Z]


def body(dims, density, potential):
    nx, ny, nz, X, Y, Z = dims
    n = nx * ny * nz
    x1, y1, z1 = X // 2, Y // 2, Z // 2
    op = coarse_operator(nx, ny, nz, float(y1 * z1), float(x1 * z1), float(x1 * y1))
    rows, rows1 = Y + 2 * R, y1 + 2 * R
    f32 = jnp.float32
    fine, one = (Y, 128), (y1, 128)
    vmem = pl.BlockSpec(memory_space=pltpu.VMEM)
    return pl.pallas_call(
        functools.partial(kernel, dims),
        out_shape=jax.ShapeDtypeStruct((X, Y, Z), f32),
        in_specs=[pl.BlockSpec(memory_space=pl.ANY)] * 3,
        out_specs=vmem,
        scratch_shapes=[
            pltpu.VMEM((n, n), f32),
            pltpu.VMEM((X, Y, Z), f32),
            pltpu.VMEM((X // 2 + 6, rows, 2 * Z), f32),
            pltpu.VMEM((X + 12, rows, 2 * Z), f32),
            pltpu.VMEM((X + 12, rows, 2 * Z), f32),
            pltpu.VMEM((X + 12, rows, 2 * Z), f32),
            pltpu.VMEM((x1 + 12, rows1, 128), f32),
            pltpu.VMEM((x1 + 12, rows1, 128), f32),
            pltpu.VMEM((x1 + 12, rows1, 128), f32),
            pltpu.VMEM((x1 // 2 + 6, rows1, 128), f32),
            pltpu.VMEM((X // 2 + 4, rows, 2 * Z), f32),
            pltpu.VMEM((n, 1, 256), f32),
            pltpu.VMEM((n, 128), f32),
        ]
        + [pltpu.VMEM(lead + s, f32) for lead in ((2,), (2, 3, 3)) for s in (fine, one, one, fine)]
        + [
            pltpu.SemaphoreType.DMA((120,)),
            pltpu.SemaphoreType.DMA((120,)),
            pltpu.SemaphoreType.DMA,
            pltpu.SemaphoreType.DMA,
            pltpu.SemaphoreType.DMA((3,)),
        ],
        compiler_params=pltpu.CompilerParams(collective_id=0, has_side_effects=True),
        name="vcycle",
    )(density, potential, op)


def solution(mesh):
    nx, ny, nz = (mesh.shape[a] for a in ("gx", "gy", "gz"))

    def run(density, potential):
        return body((nx, ny, nz) + density.shape, density, potential)

    spec = P("gx", "gy", "gz")
    return jax.shard_map(run, mesh=mesh, in_specs=(spec, spec), out_specs=spec, check_vma=False)
```

```python
import functools
import numpy as np
import jax
import jax.numpy as jnp
from jax import lax
from jax.experimental import pallas as pl
from jax.experimental.pallas import tpu as pltpu
from jax.sharding import PartitionSpec as P

SWEEPS = 2
HI = lax.Precision.HIGHEST
MESH = pl.DeviceIdType.MESH
R = 8


def table(count):
    modes = (np.arange(count) + 1) // 2
    angle = 2 * np.pi * np.outer(np.arange(count), modes) / count
    q = np.where(np.arange(count) % 2 == 1, np.cos(angle), np.sin(angle)) * np.sqrt(2 / count)
    q = np.where(2 * modes == count, np.cos(angle) / np.sqrt(count), q)
    q[:, 0] = 1 / np.sqrt(count)
    return q, 2 - 2 * np.cos(2 * np.pi * modes / count)


def coarse_operator(nx, ny, nz, wx, wy, wz):
    qx, lx = table(nx)
    qy, ly = table(ny)
    qz, lz = table(nz)
    q = np.kron(np.kron(qx, qy), qz)
    lam = wx * lx[:, None, None] + wy * ly[None, :, None] + wz * lz[None, None, :]
    lam = lam.reshape(-1)
    inv = np.concatenate([[0.0], -1.0 / lam[1:]])
    return ((q * inv) @ q.T).astype(np.float32)


def kernel(
    dims, den_hbm, pot_hbm, op_hbm, out_ref, op_ref,
    own, pm, pa, pb, den, lv, ea, eb, e2, f2, gat, cv,
    pk_p, pk_l, pk_e, pk_f, rk_p, rk_l, rk_e, rk_f,
    ssem, rsem, gs, gr, lsem,
):
    nx, ny, nz, X, Y, Z = dims
    n = nx * ny * nz
    x1, y1, z1 = X // 2, Y // 2, Z // 2
    ix, iy, iz = lax.axis_index("gx"), lax.axis_index("gy"), lax.axis_index("gz")
    me = (ix * ny + iy) * nz + iz

    def around(i, count):
        return [i] + [jnp.where(i + o >= count, i + o - count, i + o) for o in range(1, count)]

    xs, ys, zs = around(ix, nx), around(iy, ny), around(iz, nz)

    def device(o):
        if isinstance(o, int):
            return (xs[o // (ny * nz)], ys[o // nz % ny], zs[o % nz])
        ox, oy, oz = o // (ny * nz), (o // nz) % ny, o % nz
        return (lax.rem(ix + ox, nx), lax.rem(iy + oy, ny), lax.rem(iz + oz, nz))

    def each_other(step):
        if n <= 64:
            for o in range(1, n):
                step(o, 0)
        else:
            lax.fori_loop(1, n, step, 0)

    load_p = pltpu.make_async_copy(pot_hbm, own, lsem.at[0])
    load_d = pltpu.make_async_copy(den_hbm, den.at[pl.ds(6, X), pl.ds(R, Y), pl.ds(0, Z)], lsem.at[1])
    load_p.start()
    load_d.start()
    load_op = pltpu.make_async_copy(op_hbm, op_ref, lsem.at[2])
    load_op.start()

    barrier = pltpu.get_barrier_semaphore()

    def greet(o, carry):
        pl.semaphore_signal(barrier, inc=1, device_id=device(o), device_id_type=MESH)
        return carry

    near = max(nx, ny, nz) <= 5
    steps = sorted({
        (dx % nx * ny + dy % ny) * nz + dz % nz
        for dx in (-1, 0, 1) for dy in (-1, 0, 1) for dz in (-1, 0, 1)
    } - {0})
    if near:
        for o in steps:
            greet(o, 0)
    else:
        each_other(greet)
    load_p.wait()
    load_d.wait()
    odd = (
        lax.broadcasted_iota(jnp.int32, (Y, Z), 0) + lax.broadcasted_iota(jnp.int32, (Y, Z), 1)
    ) % 2 == 1
    for j in range(X // 2):
        pm[3 + j, R : R + Y, 0:Z] = jnp.where(odd, own[2 * j], own[2 * j + 1])

    sems = iter(range(200))

    def pack(items, pk):
        base = 0
        sy = items[0][3][1]
        lane = lax.broadcasted_iota(jnp.int32, (sy, 128), 1)
        head = tail = jnp.zeros((sy, 128), jnp.float32)
        for buf, h, H, (sx, sy, sz), deep in items:
            for q in range(sx):
                v = buf[H + q, R : R + sy, 0:128]
                at = base + q * deep
                inside = (lane >= at) & (lane < at + deep)
                tail = jnp.where(inside, pltpu.roll(v, (at - (sz - deep)) % 128, 1), tail)
                head = jnp.where(inside, pltpu.roll(v, at, 1) if at else v, head)
            base += sx * deep
        assert base <= 128
        pk[0] = tail
        pk[1] = head

    def once(h, H, sx):
        return nx == 2 and 2 * h > sx and H >= sx

    def exchange(items, pk, rk):
        copies = []

        def send(src, dst, dx, dy, dz):
            k = next(sems)
            to = (xs[dx], ys[dy], zs[dz])
            copy = pltpu.make_async_remote_copy(
                src_ref=src, dst_ref=dst, send_sem=ssem.at[k], recv_sem=rsem.at[k],
                device_id=to, device_id_type=MESH,
            )
            copy.start()
            copies.append(copy)

        sy = items[0][3][1]
        rows_from = {0: pl.ds(R, sy), 1: pl.ds(sy, R), -1: pl.ds(R, R)}
        rows_to = {0: pl.ds(R, sy), 1: pl.ds(0, R), -1: pl.ds(R + sy, R)}
        for dx in (1, -1, 0):
            for dy in (1, -1, 0):
                for dz in (1, -1):
                    if dx == -1 and nx == 2:
                        continue
                    side = 0 if dz == 1 else 1
                    count = R if dy else sy
                    first = sy - R if dy == 1 else 0
                    send(
                        pk.at[side, pl.ds(first, count)],
                        rk.at[side, 1 - dx, 1 - dy, pl.ds(0, count)],
                        dx, dy, dz,
                    )
                if dx == 0 and dy == 0:
                    continue
                for buf, h, H, (sx, sy, sz), deep in items:
                    if once(h, H, sx):
                        if dx == -1:
                            continue
                        h = sx if dx else h
                    p_from = {0: pl.ds(H, sx), 1: pl.ds(H + sx - h, h), -1: pl.ds(H, h)}[dx]
                    p_to = {0: pl.ds(H, sx), 1: pl.ds(H - h, h), -1: pl.ds(H + sx, h)}[dx]
                    lanes = pl.ds(0, 128)
                    send(buf.at[p_from, rows_from[dy], lanes], buf.at[p_to, rows_to[dy], lanes], dx, dy, 0)
        return functools.partial(finish, items, rk, copies)

    def finish(items, rk, copies):
        for copy in copies:
            copy.wait()
        received = {}
        for group in range(3):
            slot = 0 if nx == 2 and group == 2 else group
            for side in range(2):
                received[side, group] = jnp.concatenate(
                    [rk[side, slot, 0, 0:R], rk[side, slot, 1], rk[side, slot, 2, 0:R]], axis=0
                )
        base = 0
        for buf, h, H, (sx, sy, sz), deep in items:
            rows = sy + 2 * R
            lane = lax.broadcasted_iota(jnp.int32, (rows, 128), 1)
            wide = sz == 128
            assert not (wide and once(h, H, sx))
            put = 0 if wide else sz
            for j in range(sx + 2 * h):
                group, q = (0, sx - h + j) if j < h else ((1, j - h) if j < h + sx else (2, j - h - sx))
                at = base + q * deep
                edge = jnp.where(
                    lane >= 112,
                    pltpu.roll(received[0, group], (128 - deep - at) % 128, 1),
                    pltpu.roll(received[1, group], (put - at) % 128, 1),
                )
                if wide:
                    buf[H - h + j, :, 128:256] = edge
                else:
                    at = H - sx + q if group == 2 and once(h, H, sx) else H - h + j
                    buf[H - h + j] = jnp.where(lane < sz, buf[at], edge)
            base += sx * deep

    sixth = jnp.float32(1.0 / 6.0)

    def masks(rows, lanes):
        even = (
            lax.broadcasted_iota(jnp.int32, (rows, lanes), 0)
            + lax.broadcasted_iota(jnp.int32, (rows, lanes), 1)
        ) % 2 == 0
        return even, jnp.logical_not(even)

    def beside(a, p, c, index=lambda p: p):
        rows, lanes = c.shape
        t = a[index(p - 1)] + a[index(p + 1)]
        t = t + (pltpu.roll(c, 1, 0) + pltpu.roll(c, rows - 1, 0))
        return t + (pltpu.roll(c, 1, 1) + pltpu.roll(c, lanes - 1, 1))

    def half(a, b, s, lo, hi, H, off, colour, mask, shift=None, index=lambda p: p):
        for p in range(lo, hi):
            c = a[index(p)]
            t = beside(a, p, c, index) - s[p + off]
            if shift is not None:
                t = t + shift
            b[p] = jnp.where(mask[(p - H + colour) % 2], t * sixth, c)

    fine_mask = masks(Y + 2 * R, 2 * Z)
    one_mask = masks(y1 + 2 * R, 128)

    first = [(pm, 3, 3, (X // 2, Y, Z), 5), (den, 4, 6, (X, Y, Z), 4)]
    pack(first, pk_p)
    pl.semaphore_wait(barrier, len(steps) if near else n - 1)
    exchange(first, pk_p, rk_p)()
    for k, (a, b) in enumerate(((pm, pb), (pb, pa), (pa, pb), (pb, pa))):
        d = 4 - k
        index = (lambda p: p // 2) if k == 0 else (lambda p: p)
        half(a, b, den, 6 - d, 6 + X + d, 6, 0, k % 2, fine_mask, None, index)
    pairs = []
    total = jnp.zeros((Y, Z), jnp.float32)
    for q in range(x1):
        both = None
        for p in (6 + 2 * q, 7 + 2 * q):
            c = pa[p]
            left = (den[p] - (beside(pa, p, c) - 6.0 * c))[R : R + Y, 0:Z]
            both = left if both is None else both + left
            total = total + den[p, R : R + Y, 0:Z]
        f2[2 + q, R : R + Y, 0:Z] = jnp.where(
            odd, pa[6 + 2 * q, R : R + Y, 0:Z], pa[7 + 2 * q, R : R + Y, 0:Z]
        )
        pairs.append(both)
    def halves(shape, dim, start=0):
        i = [lax.broadcasted_iota(jnp.int32, shape, k) for k in (0, 1)]
        return jnp.where((i[dim] >> 1) + start == i[1 - dim], 1.0, 0.0).astype(jnp.float32)

    to_z, to_y = halves((Z, 128), 0), halves((x1 * y1, x1 * Y), 1)
    from_z, from_y = halves((128, 2 * Z), 1), halves((Y + 2 * R, y1 + 2 * R), 0, R // 2)
    stacked = jnp.concatenate(pairs, axis=0)
    stacked = jnp.dot(stacked, to_z, precision=HI, preferred_element_type=jnp.float32)
    one = jnp.dot(to_y, stacked, precision=HI, preferred_element_type=jnp.float32) * 0.5
    for q in range(x1):
        lv[6 + q, R : R + y1, :] = one[q * y1 : (q + 1) * y1]

    second = [(lv, 5, 6, (x1, y1, z1), 5)]
    pack(second, pk_l)
    finish_second = exchange(second, pk_l, rk_l)
    fourth = [(f2, 2, 2, (X // 2, Y, Z), 4)]
    pack(fourth, pk_f)
    finish_fourth = exchange(fourth, pk_f, rk_f)
    finish_second()
    for p in range(6 - 4, 6 + x1 + 4):
        ea[p] = jnp.where(one_mask[p % 2], lv[p] * -sixth, 0.0)
    for k, (a, b) in enumerate(((ea, eb), (eb, ea), (ea, eb))):
        d = 3 - k
        half(a, b, lv, 6 - d, 6 + x1 + d, 6, 0, (k + 1) % 2, one_mask)
    acc = jnp.zeros((y1, 128), jnp.float32)
    for p in range(6, 6 + x1):
        c = eb[p]
        acc = acc + (lv[p] - (beside(eb, p, c) - 6.0 * c))[R : R + y1]
    for j in range(x1 // 2):
        e2[3 + j, R : R + y1, :] = jnp.where(
            odd[0:y1], eb[6 + 2 * j, R : R + y1], eb[7 + 2 * j, R : R + y1]
        )
    lane = lax.broadcasted_iota(jnp.int32, (y1, 128), 1)
    acc = jnp.where(lane < z1, acc, 0.0)

    def whole_sum(v):
        return jnp.sum(jnp.sum(v, axis=0, keepdims=True), axis=1, keepdims=True)

    gat[me, :, 0:128] = jnp.broadcast_to(whole_sum(acc), (1, 128))
    gat[me, :, 128:256] = jnp.broadcast_to(whole_sum(total), (1, 128))

    def spread(o, carry):
        pltpu.make_async_remote_copy(
            src_ref=gat.at[me], dst_ref=gat.at[me], send_sem=gs, recv_sem=gr,
            device_id=device(o), device_id_type=MESH,
        ).start()
        return carry

    each_other(spread)
    third = [(e2, 3, 3, (x1 // 2, y1, z1), 6)]
    pack(third, pk_e)
    finish_third = exchange(third, pk_e, rk_e)
    finish_third()
    finish_fourth()
    others = gat.at[pl.ds(0, n - 1)]
    pltpu.make_async_copy(others, others, gs).wait()
    pltpu.make_async_copy(others, others, gr).wait()

    load_op.wait()
    values = gat[:, 0, :]
    blocks = values[:, 0:128]
    mean = jnp.sum(values[:, 128:256], axis=0, keepdims=True) / jnp.float32(n * X * Y * Z)
    blocks = blocks - jnp.sum(blocks, axis=0, keepdims=True) / jnp.float32(n)
    cv[...] = jnp.dot(op_ref[...], blocks, precision=HI, preferred_element_type=jnp.float32)
    row = lax.broadcasted_iota(jnp.int32, (y1 + 2 * R, 128), 0)
    lane = lax.broadcasted_iota(jnp.int32, (y1 + 2 * R, 128), 1)
    maps = []
    for dx in (-1, 0, 1):
        by_row = []
        for dy in (-1, 0, 1):
            vals = []
            for dz in (-1, 0, 1):
                at = (xs[dx] * ny + ys[dy]) * nz
                vals.append(cv[pl.ds(at + zs[dz], 1), :])
            by_row.append(jnp.where(lane < z1, vals[1], jnp.where(lane < (z1 + 128) // 2, vals[2], vals[0])))
        maps.append(jnp.where(row < R, by_row[0], jnp.where(row < R + y1, by_row[1], by_row[2])))
    for p in range(0, x1 + 12):
        which = 0 if p < 6 else (1 if p < 6 + x1 else 2)
        ea[p] = e2[p // 2] + (maps[which] + mean * jnp.float32(8.0 / 3.0))
    for k, (a, b) in enumerate(((ea, eb), (eb, ea), (ea, eb), (eb, ea))):
        d = 5 - k
        half(a, b, lv, 6 - d, 6 + x1 + d, 6, 0, k % 2, one_mask, 4.0 * mean)

    mean2 = jnp.concatenate([mean, mean], axis=1)
    for q in range(4, 6 + x1 + 2):
        wide = jnp.dot(ea[q], from_z, precision=HI, preferred_element_type=jnp.float32)
        wide = jnp.dot(from_y, wide, precision=HI, preferred_element_type=jnp.float32)
        wide = wide + mean2 * jnp.float32(2.0 / 3.0)
        for p in (2 * (q - 4), 2 * (q - 4) + 1):
            pb[p] = f2[p // 2] + wide
    for k, (a, b) in enumerate(((pb, pa), (pa, pb), (pb, pa))):
        d = 3 - k
        half(a, b, den, 4 - d, 4 + X + d, 4, 2, k % 2, fine_mask, mean2)
    for p in range(4, 4 + X):
        c = pa[p]
        t = (beside(pa, p, c) - den[p + 2] + mean2) * sixth
        out_ref[p - 4] = jnp.where(fine_mask[(p - 3) % 2], t, c)[R : R + Y, 0:Z]


def body(dims, density, potential):
    nx, ny, nz, X, Y, Z = dims
    n = nx * ny * nz
    x1, y1, z1 = X // 2, Y // 2, Z // 2
    op = coarse_operator(nx, ny, nz, float(y1 * z1), float(x1 * z1), float(x1 * y1))
    rows, rows1 = Y + 2 * R, y1 + 2 * R
    f32 = jnp.float32
    fine, one = (Y, 128), (y1, 128)
    vmem = pl.BlockSpec(memory_space=pltpu.VMEM)
    return pl.pallas_call(
        functools.partial(kernel, dims),
        out_shape=jax.ShapeDtypeStruct((X, Y, Z), f32),
        in_specs=[pl.BlockSpec(memory_space=pl.ANY)] * 3,
        out_specs=vmem,
        scratch_shapes=[
            pltpu.VMEM((n, n), f32),
            pltpu.VMEM((X, Y, Z), f32),
            pltpu.VMEM((X // 2 + 6, rows, 2 * Z), f32),
            pltpu.VMEM((X + 12, rows, 2 * Z), f32),
            pltpu.VMEM((X + 12, rows, 2 * Z), f32),
            pltpu.VMEM((X + 12, rows, 2 * Z), f32),
            pltpu.VMEM((x1 + 12, rows1, 128), f32),
            pltpu.VMEM((x1 + 12, rows1, 128), f32),
            pltpu.VMEM((x1 + 12, rows1, 128), f32),
            pltpu.VMEM((x1 // 2 + 6, rows1, 128), f32),
            pltpu.VMEM((X // 2 + 4, rows, 2 * Z), f32),
            pltpu.VMEM((n, 1, 256), f32),
            pltpu.VMEM((n, 128), f32),
        ]
        + [pltpu.VMEM(lead + s, f32) for lead in ((2,), (2, 3, 3)) for s in (fine, one, one, fine)]
        + [
            pltpu.SemaphoreType.DMA((120,)),
            pltpu.SemaphoreType.DMA((120,)),
            pltpu.SemaphoreType.DMA,
            pltpu.SemaphoreType.DMA,
            pltpu.SemaphoreType.DMA((3,)),
        ],
        compiler_params=pltpu.CompilerParams(collective_id=0, has_side_effects=True),
        name="vcycle",
    )(density, potential, op)


def solution(mesh):
    nx, ny, nz = (mesh.shape[a] for a in ("gx", "gy", "gz"))

    def run(density, potential):
        return body((nx, ny, nz) + density.shape, density, potential)

    spec = P("gx", "gy", "gz")
    return jax.shard_map(run, mesh=mesh, in_specs=(spec, spec), out_specs=spec, check_vma=False)
```

```python
import functools
import numpy as np
import jax
import jax.numpy as jnp
from jax import lax
from jax.experimental import pallas as pl
from jax.experimental.pallas import tpu as pltpu
from jax.sharding import PartitionSpec as P

SWEEPS = 2
HI = lax.Precision.HIGHEST
MESH = pl.DeviceIdType.MESH
R = 8


def table(count):
    modes = (np.arange(count) + 1) // 2
    angle = 2 * np.pi * np.outer(np.arange(count), modes) / count
    q = np.where(np.arange(count) % 2 == 1, np.cos(angle), np.sin(angle)) * np.sqrt(2 / count)
    q = np.where(2 * modes == count, np.cos(angle) / np.sqrt(count), q)
    q[:, 0] = 1 / np.sqrt(count)
    return q, 2 - 2 * np.cos(2 * np.pi * modes / count)


def coarse_operator(nx, ny, nz, wx, wy, wz):
    qx, lx = table(nx)
    qy, ly = table(ny)
    qz, lz = table(nz)
    q = np.kron(np.kron(qx, qy), qz)
    lam = wx * lx[:, None, None] + wy * ly[None, :, None] + wz * lz[None, None, :]
    lam = lam.reshape(-1)
    inv = np.concatenate([[0.0], -1.0 / lam[1:]])
    return ((q * inv) @ q.T).astype(np.float32)


def kernel(
    dims, den_hbm, pot_hbm, op_hbm, out_ref, op_ref,
    own, pm, pa, pb, den, lv, ea, eb, e2, f2, gat, cv,
    pk_p, pk_l, pk_e, pk_f, rk_p, rk_l, rk_e, rk_f,
    ssem, rsem, gs, gr, lsem,
):
    nx, ny, nz, X, Y, Z = dims
    n = nx * ny * nz
    x1, y1, z1 = X // 2, Y // 2, Z // 2
    ix, iy, iz = lax.axis_index("gx"), lax.axis_index("gy"), lax.axis_index("gz")
    me = (ix * ny + iy) * nz + iz

    def around(i, count):
        return [i] + [jnp.where(i + o >= count, i + o - count, i + o) for o in range(1, count)]

    xs, ys, zs = around(ix, nx), around(iy, ny), around(iz, nz)

    def device(o):
        if isinstance(o, int):
            return (xs[o // (ny * nz)], ys[o // nz % ny], zs[o % nz])
        ox, oy, oz = o // (ny * nz), (o // nz) % ny, o % nz
        return (lax.rem(ix + ox, nx), lax.rem(iy + oy, ny), lax.rem(iz + oz, nz))

    def each_other(step):
        if n <= 64:
            for o in range(1, n):
                step(o, 0)
        else:
            lax.fori_loop(1, n, step, 0)

    load_p = pltpu.make_async_copy(pot_hbm, own, lsem.at[0])
    load_d = pltpu.make_async_copy(den_hbm, den.at[pl.ds(6, X), pl.ds(R, Y), pl.ds(0, Z)], lsem.at[1])
    load_p.start()
    load_d.start()
    load_op = pltpu.make_async_copy(op_hbm, op_ref, lsem.at[2])
    load_op.start()

    barrier = pltpu.get_barrier_semaphore()

    def greet(o, carry):
        pl.semaphore_signal(barrier, inc=1, device_id=device(o), device_id_type=MESH)
        return carry

    near = max(nx, ny, nz) <= 5
    steps = sorted({
        (dx % nx * ny + dy % ny) * nz + dz % nz
        for dx in (-1, 0, 1) for dy in (-1, 0, 1) for dz in (-1, 0, 1)
    } - {0})
    if near:
        for o in steps:
            greet(o, 0)
    else:
        each_other(greet)
    load_p.wait()
    load_d.wait()
    odd = (
        lax.broadcasted_iota(jnp.int32, (Y, Z), 0) + lax.broadcasted_iota(jnp.int32, (Y, Z), 1)
    ) % 2 == 1
    for j in range(X // 2):
        pm[3 + j, R : R + Y, 0:Z] = jnp.where(odd, own[2 * j], own[2 * j + 1])

    sems = iter(range(200))

    def pack(items, pk):
        base = 0
        sy = items[0][3][1]
        lane = lax.broadcasted_iota(jnp.int32, (sy, 128), 1)
        head = tail = jnp.zeros((sy, 128), jnp.float32)
        for buf, h, H, (sx, sy, sz), deep in items:
            for q in range(sx):
                v = buf[H + q, R : R + sy, 0:128]
                at = base + q * deep
                inside = (lane >= at) & (lane < at + deep)
                tail = jnp.where(inside, pltpu.roll(v, (at - (sz - deep)) % 128, 1), tail)
                head = jnp.where(inside, pltpu.roll(v, at, 1) if at else v, head)
            base += sx * deep
        assert base <= 128
        pk[0] = tail
        pk[1] = head

    def once(h, H, sx):
        return nx == 2 and 2 * h > sx and H >= sx

    def exchange(items, pk, rk):
        copies = []

        def send(src, dst, dx, dy, dz):
            k = next(sems)
            to = (xs[dx], ys[dy], zs[dz])
            copy = pltpu.make_async_remote_copy(
                src_ref=src, dst_ref=dst, send_sem=ssem.at[k], recv_sem=rsem.at[k],
                device_id=to, device_id_type=MESH,
            )
            copy.start()
            copies.append(copy)

        sy = items[0][3][1]
        rows_from = {0: pl.ds(R, sy), 1: pl.ds(sy, R), -1: pl.ds(R, R)}
        rows_to = {0: pl.ds(R, sy), 1: pl.ds(0, R), -1: pl.ds(R + sy, R)}
        for dx in (1, -1, 0):
            for dy in (1, -1, 0):
                for dz in (1, -1):
                    if dx == -1 and nx == 2:
                        continue
                    side = 0 if dz == 1 else 1
                    count = R if dy else sy
                    first = sy - R if dy == 1 else 0
                    send(
                        pk.at[side, pl.ds(first, count)],
                        rk.at[side, 1 - dx, 1 - dy, pl.ds(0, count)],
                        dx, dy, dz,
                    )
                if dx == 0 and dy == 0:
                    continue
                for buf, h, H, (sx, sy, sz), deep in items:
                    if once(h, H, sx):
                        if dx == -1:
                            continue
                        h = sx if dx else h
                    p_from = {0: pl.ds(H, sx), 1: pl.ds(H + sx - h, h), -1: pl.ds(H, h)}[dx]
                    p_to = {0: pl.ds(H, sx), 1: pl.ds(H - h, h), -1: pl.ds(H + sx, h)}[dx]
                    lanes = pl.ds(0, 128)
                    send(buf.at[p_from, rows_from[dy], lanes], buf.at[p_to, rows_to[dy], lanes], dx, dy, 0)
        return functools.partial(finish, items, rk, copies)

    def finish(items, rk, copies):
        for copy in copies:
            copy.wait()
        received = {}
        for group in range(3):
            slot = 0 if nx == 2 and group == 2 else group
            for side in range(2):
                received[side, group] = jnp.concatenate(
                    [rk[side, slot, 0, 0:R], rk[side, slot, 1], rk[side, slot, 2, 0:R]], axis=0
                )
        base = 0
        for buf, h, H, (sx, sy, sz), deep in items:
            rows = sy + 2 * R
            lane = lax.broadcasted_iota(jnp.int32, (rows, 128), 1)
            wide = sz == 128
            assert not (wide and once(h, H, sx))
            put = 0 if wide else sz
            for j in range(sx + 2 * h):
                group, q = (0, sx - h + j) if j < h else ((1, j - h) if j < h + sx else (2, j - h - sx))
                at = base + q * deep
                edge = jnp.where(
                    lane >= 112,
                    pltpu.roll(received[0, group], (128 - deep - at) % 128, 1),
                    pltpu.roll(received[1, group], (put - at) % 128, 1),
                )
                if wide:
                    buf[H - h + j, :, 128:256] = edge
                else:
                    at = H - sx + q if group == 2 and once(h, H, sx) else H - h + j
                    buf[H - h + j] = jnp.where(lane < sz, buf[at], edge)
            base += sx * deep

    sixth = jnp.float32(1.0 / 6.0)

    def masks(rows, lanes):
        even = (
            lax.broadcasted_iota(jnp.int32, (rows, lanes), 0)
            + lax.broadcasted_iota(jnp.int32, (rows, lanes), 1)
        ) % 2 == 0
        return even, jnp.logical_not(even)

    def beside(a, p, c, index=lambda p: p):
        rows, lanes = c.shape
        t = a[index(p - 1)] + a[index(p + 1)]
        t = t + (pltpu.roll(c, 1, 0) + pltpu.roll(c, rows - 1, 0))
        return t + (pltpu.roll(c, 1, 1) + pltpu.roll(c, lanes - 1, 1))

    def half(a, b, s, lo, hi, H, off, colour, mask, shift=None, index=lambda p: p):
        for p in range(lo, hi):
            c = a[index(p)]
            t = beside(a, p, c, index) - s[p + off]
            if shift is not None:
                t = t + shift
            b[p] = jnp.where(mask[(p - H + colour) % 2], t * sixth, c)

    fine_mask = masks(Y + 2 * R, 2 * Z)
    one_mask = masks(y1 + 2 * R, 128)

    first = [(pm, 3, 3, (X // 2, Y, Z), 5), (den, 4, 6, (X, Y, Z), 4)]
    pack(first, pk_p)
    pl.semaphore_wait(barrier, len(steps) if near else n - 1)
    exchange(first, pk_p, rk_p)()
    for k, (a, b) in enumerate(((pm, pb), (pb, pa), (pa, pb), (pb, pa))):
        d = 4 - k
        index = (lambda p: p // 2) if k == 0 else (lambda p: p)
        half(a, b, den, 6 - d, 6 + X + d, 6, 0, k % 2, fine_mask, None, index)
    pairs = []
    total = jnp.zeros((Y, Z), jnp.float32)
    for q in range(x1):
        both = None
        for p in (6 + 2 * q, 7 + 2 * q):
            c = pa[p]
            left = (den[p] - (beside(pa, p, c) - 6.0 * c))[R : R + Y, 0:Z]
            both = left if both is None else both + left
            total = total + den[p, R : R + Y, 0:Z]
        f2[2 + q, R : R + Y, 0:Z] = jnp.where(
            odd, pa[6 + 2 * q, R : R + Y, 0:Z], pa[7 + 2 * q, R : R + Y, 0:Z]
        )
        pairs.append(both)
    def halves(shape, dim, start=0):
        i = [lax.broadcasted_iota(jnp.int32, shape, k) for k in (0, 1)]
        return jnp.where((i[dim] >> 1) + start == i[1 - dim], 1.0, 0.0).astype(jnp.float32)

    to_z, to_y = halves((Z, 128), 0), halves((x1 * y1, x1 * Y), 1)
    from_z, from_y = halves((128, 2 * Z), 1), halves((Y + 2 * R, y1 + 2 * R), 0, R // 2)
    stacked = jnp.concatenate(pairs, axis=0)
    stacked = jnp.dot(stacked, to_z, precision=HI, preferred_element_type=jnp.float32)
    one = jnp.dot(to_y, stacked, precision=HI, preferred_element_type=jnp.float32) * 0.5
    for q in range(x1):
        lv[6 + q, R : R + y1, :] = one[q * y1 : (q + 1) * y1]

    second = [(lv, 5, 6, (x1, y1, z1), 5)]
    pack(second, pk_l)
    finish_second = exchange(second, pk_l, rk_l)
    fourth = [(f2, 2, 2, (X // 2, Y, Z), 4)]
    pack(fourth, pk_f)
    finish_fourth = exchange(fourth, pk_f, rk_f)
    def whole_sum(v):
        return jnp.sum(jnp.sum(v, axis=0, keepdims=True), axis=1, keepdims=True)

    gat[me, :, 128:256] = jnp.broadcast_to(whole_sum(total), (1, 128))
    finish_second()
    for p in range(6 - 4, 6 + x1 + 4):
        ea[p] = jnp.where(one_mask[p % 2], lv[p] * -sixth, 0.0)
    for k, (a, b) in enumerate(((ea, eb), (eb, ea), (ea, eb))):
        d = 3 - k
        half(a, b, lv, 6 - d, 6 + x1 + d, 6, 0, (k + 1) % 2, one_mask)
    acc = jnp.zeros((y1, 128), jnp.float32)
    for p in range(6, 6 + x1):
        c = eb[p]
        acc = acc + (lv[p] - (beside(eb, p, c) - 6.0 * c))[R : R + y1]
    for j in range(x1 // 2):
        e2[3 + j, R : R + y1, :] = jnp.where(
            odd[0:y1], eb[6 + 2 * j, R : R + y1], eb[7 + 2 * j, R : R + y1]
        )
    lane = lax.broadcasted_iota(jnp.int32, (y1, 128), 1)
    acc = jnp.where(lane < z1, acc, 0.0)

    gat[me, :, 0:128] = jnp.broadcast_to(whole_sum(acc), (1, 128))

    def spread(o, carry):
        pltpu.make_async_remote_copy(
            src_ref=gat.at[me], dst_ref=gat.at[me], send_sem=gs, recv_sem=gr,
            device_id=device(o), device_id_type=MESH,
        ).start()
        return carry

    each_other(spread)
    third = [(e2, 3, 3, (x1 // 2, y1, z1), 6)]
    pack(third, pk_e)
    finish_third = exchange(third, pk_e, rk_e)
    finish_fourth()
    finish_third()
    others = gat.at[pl.ds(0, n - 1)]
    pltpu.make_async_copy(others, others, gs).wait()
    pltpu.make_async_copy(others, others, gr).wait()

    load_op.wait()
    values = gat[:, 0, :]
    blocks = values[:, 0:128]
    mean = jnp.sum(values[:, 128:256], axis=0, keepdims=True) / jnp.float32(n * X * Y * Z)
    blocks = blocks - jnp.sum(blocks, axis=0, keepdims=True) / jnp.float32(n)
    cv[...] = jnp.dot(op_ref[...], blocks, precision=HI, preferred_element_type=jnp.float32)
    row = lax.broadcasted_iota(jnp.int32, (y1 + 2 * R, 128), 0)
    lane = lax.broadcasted_iota(jnp.int32, (y1 + 2 * R, 128), 1)
    maps = []
    for dx in (-1, 0, 1):
        by_row = []
        for dy in (-1, 0, 1):
            vals = []
            for dz in (-1, 0, 1):
                at = (xs[dx] * ny + ys[dy]) * nz
                vals.append(cv[pl.ds(at + zs[dz], 1), :])
            by_row.append(jnp.where(lane < z1, vals[1], jnp.where(lane < (z1 + 128) // 2, vals[2], vals[0])))
        maps.append(jnp.where(row < R, by_row[0], jnp.where(row < R + y1, by_row[1], by_row[2])))
    for p in range(0, x1 + 12):
        which = 0 if p < 6 else (1 if p < 6 + x1 else 2)
        ea[p] = e2[p // 2] + (maps[which] + mean * jnp.float32(8.0 / 3.0))
    for k, (a, b) in enumerate(((ea, eb), (eb, ea), (ea, eb), (eb, ea))):
        d = 5 - k
        half(a, b, lv, 6 - d, 6 + x1 + d, 6, 0, k % 2, one_mask, 4.0 * mean)

    mean2 = jnp.concatenate([mean, mean], axis=1)
    for q in range(4, 6 + x1 + 2):
        wide = jnp.dot(ea[q], from_z, precision=HI, preferred_element_type=jnp.float32)
        wide = jnp.dot(from_y, wide, precision=HI, preferred_element_type=jnp.float32)
        wide = wide + mean2 * jnp.float32(2.0 / 3.0)
        for p in (2 * (q - 4), 2 * (q - 4) + 1):
            pb[p] = f2[p // 2] + wide
    for k, (a, b) in enumerate(((pb, pa), (pa, pb), (pb, pa))):
        d = 3 - k
        half(a, b, den, 4 - d, 4 + X + d, 4, 2, k % 2, fine_mask, mean2)
    for p in range(4, 4 + X):
        c = pa[p]
        t = (beside(pa, p, c) - den[p + 2] + mean2) * sixth
        out_ref[p - 4] = jnp.where(fine_mask[(p - 3) % 2], t, c)[R : R + Y, 0:Z]


def body(dims, density, potential):
    nx, ny, nz, X, Y, Z = dims
    n = nx * ny * nz
    x1, y1, z1 = X // 2, Y // 2, Z // 2
    op = coarse_operator(nx, ny, nz, float(y1 * z1), float(x1 * z1), float(x1 * y1))
    rows, rows1 = Y + 2 * R, y1 + 2 * R
    f32 = jnp.float32
    fine, one = (Y, 128), (y1, 128)
    vmem = pl.BlockSpec(memory_space=pltpu.VMEM)
    return pl.pallas_call(
        functools.partial(kernel, dims),
        out_shape=jax.ShapeDtypeStruct((X, Y, Z), f32),
        in_specs=[pl.BlockSpec(memory_space=pl.ANY)] * 3,
        out_specs=vmem,
        scratch_shapes=[
            pltpu.VMEM((n, n), f32),
            pltpu.VMEM((X, Y, Z), f32),
            pltpu.VMEM((X // 2 + 6, rows, 2 * Z), f32),
            pltpu.VMEM((X + 12, rows, 2 * Z), f32),
            pltpu.VMEM((X + 12, rows, 2 * Z), f32),
            pltpu.VMEM((X + 12, rows, 2 * Z), f32),
            pltpu.VMEM((x1 + 12, rows1, 128), f32),
            pltpu.VMEM((x1 + 12, rows1, 128), f32),
            pltpu.VMEM((x1 + 12, rows1, 128), f32),
            pltpu.VMEM((x1 // 2 + 6, rows1, 128), f32),
            pltpu.VMEM((X // 2 + 4, rows, 2 * Z), f32),
            pltpu.VMEM((n, 1, 256), f32),
            pltpu.VMEM((n, 128), f32),
        ]
        + [pltpu.VMEM(lead + s, f32) for lead in ((2,), (2, 3, 3)) for s in (fine, one, one, fine)]
        + [
            pltpu.SemaphoreType.DMA((120,)),
            pltpu.SemaphoreType.DMA((120,)),
            pltpu.SemaphoreType.DMA,
            pltpu.SemaphoreType.DMA,
            pltpu.SemaphoreType.DMA((3,)),
        ],
        compiler_params=pltpu.CompilerParams(collective_id=0, has_side_effects=True),
        name="vcycle",
    )(density, potential, op)


def solution(mesh):
    nx, ny, nz = (mesh.shape[a] for a in ("gx", "gy", "gz"))

    def run(density, potential):
        return body((nx, ny, nz) + density.shape, density, potential)

    spec = P("gx", "gy", "gz")
    return jax.shard_map(run, mesh=mesh, in_specs=(spec, spec), out_specs=spec, check_vma=False)
```
